32 devices in a mesh: dp: 4 (over x, y), tp: 8 (over z, core).
Axes of the slice: x: 2, y: 2, z: 4, core: 2. Of those that a mesh axis runs over, the one named last changes fastest.
Arguments:
- x: bfloat16 [256, 3072], P('dp'), parts along dimension 0
- k_cache: bfloat16 [256, 1024, 32, 96], P('dp', None, 'tp'), parts along dimension 0
- v_cache: bfloat16 [256, 1024, 32, 96], P('dp', None, 'tp'), parts along dimension 0
- gain_a: bfloat16 [3072], replicated
- wq: bfloat16 [3072, 3072], P(None, 'tp')
- wo: bfloat16 [3072, 3072], P('tp')
- gain_m: bfloat16 [3072], replicated
- w_gate: bfloat16 [3072, 8192], P(None, 'tp')
- w_up: bfloat16 [3072, 8192], P(None, 'tp')
- w_down: bfloat16 [8192, 3072], P('tp')
Outputs:
- output: bfloat16 [256, 3072], P('dp'), parts along dimension 0
There are 4 independent parts. The reference program is written for one: setup_inputs(seed, part) draws one part's arguments, and reference() takes and returns one part's arrays. A program takes and returns all parts, laid end to end along the dimension named above; an argument that names none is the same for every part.
All inputs are finite; a program needn't handle non-finite values.
Results may differ from the reference program's by a relative error of at most 0.017.
Values are sent between devices in bfloat16 or wider.
A program may use at most 2 GiB of HBM per device.

```python
import jax
import jax.numpy as jnp
from jax import lax

BATCH = 64
CACHE = 1024
D = 3072
HEADS = 32
KV_HEADS = 32
HEAD = 96
FF = 8192
THETA = 10000


def setup_inputs(seed: int = 0, part: int = 0) -> dict:
    kx, kc, kw, kn, kq, ko, km, kg, ku, kd = jax.random.split(jax.random.key(seed), 10)
    kx, kc, kw = (jax.random.fold_in(k, part) for k in (kx, kc, kw))

    def weights(key, rows, columns):
        return jax.random.normal(key, (rows, columns), jnp.float32) * rows**-0.5

    drawn = {
        "x": jax.random.normal(kx, (BATCH, D), jnp.float32),
        "k_cache": 2 * jax.random.normal(kc, (BATCH, CACHE, KV_HEADS, HEAD), jnp.float32),
        "v_cache": 4 * jax.random.normal(kw, (BATCH, CACHE, KV_HEADS, HEAD), jnp.float32),
        "gain_a": 1 + 0.1 * jax.random.normal(kn, (D,), jnp.float32),
        "wq": 2 * weights(kq, D, HEADS * HEAD),
        "wo": weights(ko, HEADS * HEAD, D),
        "gain_m": 1 + 0.1 * jax.random.normal(km, (D,), jnp.float32),
        "w_gate": weights(kg, D, FF),
        "w_up": weights(ku, D, FF),
        "w_down": 2 * weights(kd, FF, D),
    }
    return {k: v.astype(jnp.bfloat16) for k, v in drawn.items()}


def normed(x, gain):
    wide = x.astype(jnp.float32)
    scale = lax.rsqrt(jnp.mean(wide * wide, -1, keepdims=True) + 1e-6)
    return (wide * scale * gain.astype(jnp.float32)).astype(jnp.bfloat16)


def turned(t, place, theta):
    half = t.shape[-1] // 2
    angle = place.astype(jnp.float32)[:, None] * theta ** (-jnp.arange(half, dtype=jnp.float32) / half)
    cos, sin = jnp.cos(angle)[:, None], jnp.sin(angle)[:, None]
    a, b = t[..., :half].astype(jnp.float32), t[..., half:].astype(jnp.float32)
    return jnp.concatenate([a * cos - b * sin, b * cos + a * sin], -1).astype(jnp.bfloat16)


def matmul(a, w):
    return jnp.dot(a, w, preferred_element_type=jnp.float32).astype(jnp.bfloat16)


def einsum(form, a, b):
    return jnp.einsum(form, a.astype(jnp.float32), b.astype(jnp.float32))


def seen_by(a, wq, k_cache, v_cache, head, theta):
    batch, cache, kv_heads = k_cache.shape[:3]
    place = jnp.full((batch,), cache - 1)
    q = turned(matmul(a, wq).reshape(batch, -1, head), place, theta).reshape(batch, kv_heads, -1, head)
    scores = einsum("bgsd,bugd->bgsu", q, k_cache) * head**-0.5
    weights = jax.nn.softmax(scores, -1).astype(jnp.bfloat16)
    return einsum("bgsu,bugd->bgsd", weights, v_cache).astype(jnp.bfloat16).reshape(batch, -1)


def hidden_of(b, w_gate, w_up):
    gate = jnp.dot(b, w_gate, preferred_element_type=jnp.float32)
    up = jnp.dot(b, w_up, preferred_element_type=jnp.float32)
    return (jax.nn.silu(gate) * up).astype(jnp.bfloat16)


def reference(x, k_cache, v_cache, gain_a, wq, wo, gain_m, w_gate, w_up, w_down):
    seen = seen_by(normed(x, gain_a), wq, k_cache, v_cache, HEAD, THETA)
    h = (x.astype(jnp.float32) + jnp.dot(seen, wo, preferred_element_type=jnp.float32)).astype(jnp.bfloat16)
    hidden = hidden_of(normed(h, gain_m), w_gate, w_up)
    return (h.astype(jnp.float32) + jnp.dot(hidden, w_down, preferred_element_type=jnp.float32)).astype(jnp.bfloat16)
```

```python
import functools

import jax
import jax.numpy as jnp
import numpy as np
from jax import lax
from jax.experimental import pallas as pl
from jax.experimental.pallas import tpu as pltpu
from jax.sharding import PartitionSpec as P

HEAD = 96
THETA = 10000
N = 8
ROWS, D = 64, 3072
COLS = D // N
HEADS = 4
QD = HEADS * HEAD
CACHE = 1024
FF = 1024
SEQS = 4
CHUNKS = ROWS // SEQS
SLOTS = 4
GROUP = 16
GROUPS = ROWS // GROUP
PER = GROUP // SEQS
MTILE = 256
F32, BF16 = jnp.float32, jnp.bfloat16


def dot(a, b):
    return jnp.dot(a, b, preferred_element_type=F32)


def kernel(x_h, k_h, v_h, ga_h, wq_h, wo_h, gm_h, wg_h, wu_h, wd_h, cs_h, out_h,
           x_v, ga_v, gm_v, cs_v, wq_v, wo_v, wg_v, wu_v, wd_v, k_v, v_v,
           a_v, q_s, p_s, seen_s, term_s, tsend, trecv, h_v, hid_v, ysend, yrecv, y_v,
           in_sem, k_sem, v_sem, w_sem, out_sem, rs_s, rs_r, ag_s, ag_r, rs2_s, rs2_r, ag2_s, ag2_r):
    me = lax.axis_index("tp")

    def peer(k):
        return lax.rem(me + k, N)

    def local(src, dst, sem):
        return pltpu.make_async_copy(src, dst, sem)

    x_in = local(x_h, x_v, in_sem.at[0])
    ga_in = local(ga_h, ga_v, in_sem.at[1])
    cs_in = local(cs_h, cs_v, in_sem.at[2])
    wq_in = local(wq_h, wq_v, in_sem.at[3])
    wo_in = local(wo_h, wo_v, in_sem.at[4])
    gm_in = local(gm_h, gm_v, in_sem.at[5])

    def k_in(c):
        s = lax.rem(c, SLOTS)
        return local(k_h.at[c], k_v.at[s], k_sem.at[s])

    def v_in(c):
        s = lax.rem(c, SLOTS)
        return local(v_h.at[c], v_v.at[s], v_sem.at[s])

    def w_in(n):
        cols = pl.ds(n * MTILE, MTILE)
        return (local(wg_h.at[:, cols], wg_v.at[:, cols], w_sem.at[0, n]),
                local(wu_h.at[:, cols], wu_v.at[:, cols], w_sem.at[1, n]))

    wd_in = local(wd_h, wd_v, in_sem.at[6])

    x_in.start()
    ga_in.start()
    cs_in.start()
    wq_in.start()
    for c in range(SLOTS):
        k_in(c).start()
        v_in(c).start()
        if c == 0:
            wo_in.start()
            gm_in.start()

    barrier = pltpu.get_barrier_semaphore()
    for k in range(1, N):
        pl.semaphore_signal(barrier, inc=1, device_id={"tp": peer(k)}, device_id_type=pl.DeviceIdType.MESH)
    pl.semaphore_wait(barrier, N - 1)

    x_in.wait()
    ga_in.wait()

    def norm_x(i, _):
        rows = pl.ds(pl.multiple_of(i * GROUP, GROUP), GROUP)
        wide = x_v[rows, :].astype(F32)
        scale = lax.rsqrt(jnp.mean(wide * wide, -1, keepdims=True) + 1e-6)
        a_v[rows, :] = (wide * scale * ga_v[...].astype(F32)).astype(BF16)
        return 0

    lax.fori_loop(0, GROUPS, norm_x, 0)
    wq_in.wait()
    cs_in.wait()
    q = dot(a_v[...], wq_v[...]).astype(BF16).astype(F32)
    lane = lax.broadcasted_iota(jnp.int32, (ROWS, QD), 1)
    ahead = pltpu.roll(q, QD - HEAD // 2, 1)
    behind = pltpu.roll(q, HEAD // 2, 1)
    turn = jnp.where(lax.rem(lane, HEAD) < HEAD // 2, -ahead, behind)
    q_s[...] = (q * cs_v[0:1, :] + turn * cs_v[1:2, :]).astype(BF16).astype(F32)

    row16 = lax.broadcasted_iota(jnp.int32, (SEQS * HEADS, QD), 0)
    lane16 = lax.broadcasted_iota(jnp.int32, (SEQS * HEADS, QD), 1)
    masks = [row16 == i * HEADS + lane16 // HEAD for i in range(SEQS)]

    def weights_of(c):
        k_in(c).wait()
        parts = []
        for i in range(SEQS):
            row = q_s[pl.ds(c * SEQS + i, 1), :]
            parts.append(jnp.where(masks[i], jnp.broadcast_to(row, (SEQS * HEADS, QD)), 0.0))
        qd = jnp.concatenate(parts, 1).astype(BF16)
        s = dot(qd, k_v[lax.rem(c, SLOTS)]) * HEAD**-0.5
        e = jnp.exp(s - jnp.max(s, -1, keepdims=True))
        return (e * (1.0 / jnp.sum(e, -1, keepdims=True))).astype(BF16)

    def values_of(c, p):
        o = lax.dot_general(p, v_v[lax.rem(c, SLOTS)], (((1,), (1,)), ((), ())), preferred_element_type=F32)
        for i in range(SEQS):
            part = jnp.where(masks[i], o[:, i * QD:(i + 1) * QD], 0.0)
            seen_s[pl.ds(c * SEQS + i, 1), :] = jnp.sum(part, 0, keepdims=True)

    def group_rows(g):
        return pl.ds(pl.multiple_of(g * GROUP, GROUP), GROUP)

    def rs_copy(g, k):
        return pltpu.make_async_remote_copy(
            src_ref=tsend.at[g, peer(k)], dst_ref=trecv.at[g, k], send_sem=rs_s.at[g, k], recv_sem=rs_r.at[g, k],
            device_id={"tp": peer(k)}, device_id_type=pl.DeviceIdType.MESH)

    def ag_copy(g, k):
        block = h_v.at[me, group_rows(g), :]
        return pltpu.make_async_remote_copy(
            src_ref=block, dst_ref=block, send_sem=ag_s.at[g, k], recv_sem=ag_r.at[g, k],
            device_id={"tp": peer(k)}, device_id_type=pl.DeviceIdType.MESH)

    def send_terms(g):
        seen = seen_s[group_rows(g), :].astype(BF16)
        term = dot(seen, wo_v[...])
        for j in range(N):
            block = term[:, j * COLS:(j + 1) * COLS]
            term_s[g, j] = block
            tsend[g, j] = block.astype(BF16)
        for k in range(1, N):
            rs_copy(g, k).start()

    def finish_h(g):
        rows = group_rows(g)
        total = term_s[g, me]
        for k in range(1, N):
            rs_copy(g, k).wait_recv()
            total = total + trecv[g, k].astype(F32)
        mine = x_v[rows, pl.ds(pl.multiple_of(me * COLS, COLS), COLS)].astype(F32)
        h_v[me, rows, :] = (mine + total).astype(BF16)
        for k in range(1, N):
            ag_copy(g, k).start()

    def norm_h(g):
        rows = group_rows(g)
        for k in range(1, N):
            ag_copy(g, k).wait_recv()
        wide = [h_v[j, rows, :].astype(F32) for j in range(N)]
        square = sum(jnp.sum(w * w, -1, keepdims=True) for w in wide)
        scale = lax.rsqrt(square / D + 1e-6)
        for j in range(N):
            cols = slice(j * COLS, (j + 1) * COLS)
            a_v[rows, cols] = (wide[j] * scale * gm_v[:, cols].astype(F32)).astype(BF16)

    p_s[...] = weights_of(0)
    wo_in.wait()
    gm_in.wait()

    def chunk(c, _):
        @pl.when(c + SLOTS - 1 < CHUNKS)
        def _():
            k_in(c + SLOTS - 1).start()

        @pl.when(jnp.logical_and(c >= 2, c + SLOTS - 2 < CHUNKS))
        def _():
            v_in(c + SLOTS - 2).start()

        @pl.when(c == CHUNKS - SLOTS + 1)
        def _():
            for n in range(FF // MTILE):
                for w in w_in(n):
                    w.start()
            wd_in.start()

        v_in(c - 1).wait()
        p = p_s[...]
        p_s[...] = weights_of(c)
        values_of(c - 1, p)

        @pl.when(lax.rem(c, PER) == 0)
        def _():
            send_terms(c // PER - 1)

        @pl.when(jnp.logical_and(lax.rem(c, PER) == PER - 1, c >= 2 * PER - 1))
        def _():
            finish_h(c // PER - 1)

        return 0

    lax.fori_loop(1, CHUNKS, chunk, 0)
    v_in(CHUNKS - 1).wait()
    values_of(CHUNKS - 1, p_s[...])
    send_terms(GROUPS - 1)
    lax.fori_loop(0, GROUPS - 1, lambda g, _: (norm_h(g), 0)[1], 0)
    finish_h(GROUPS - 1)
    norm_h(GROUPS - 1)

    def hidden(n, _):
        for w in w_in(n):
            w.wait()
        cols = pl.ds(pl.multiple_of(n * MTILE, MTILE), MTILE)
        gate = dot(a_v[...], wg_v[:, cols])
        up = dot(a_v[...], wu_v[:, cols])
        hid_v[:, cols] = (jax.nn.silu(gate) * up).astype(BF16)
        return 0

    lax.fori_loop(0, FF // MTILE, hidden, 0)
    wd_in.wait()

    def rs2_copy(k):
        return pltpu.make_async_remote_copy(
            src_ref=ysend.at[k], dst_ref=yrecv.at[k], send_sem=rs2_s.at[k], recv_sem=rs2_r.at[k],
            device_id={"tp": peer(k)}, device_id_type=pl.DeviceIdType.MESH)

    def ag2_copy(k):
        return pltpu.make_async_remote_copy(
            src_ref=y_v.at[me], dst_ref=y_v.at[me], send_sem=ag2_s.at[k], recv_sem=ag2_r.at[k],
            device_id={"tp": peer(k)}, device_id_type=pl.DeviceIdType.MESH)

    def down(j):
        return dot(hid_v[...], wd_v[:, pl.ds(pl.multiple_of(j * COLS, COLS), COLS)])

    for k in range(1, N):
        ysend[k] = down(peer(k)).astype(BF16)
        rs2_copy(k).start()
    total = down(me)
    for k in range(1, N):
        rs2_copy(k).wait_recv()
        total = total + yrecv[k].astype(F32)
    y_v[me] = (h_v[me].astype(F32) + total).astype(BF16)
    for k in range(1, N):
        ag2_copy(k).start()

    def out_copy(j):
        return local(y_v.at[j], out_h.at[:, pl.ds(pl.multiple_of(j * COLS, COLS), COLS)], out_sem.at[j])

    out_copy(me).start()
    for k in range(1, N):
        ag2_copy(k).wait_recv()
        out_copy(lax.rem(me + N - k, N)).start()
    for j in range(N):
        out_copy(j).wait()

    def sent(g, _):
        for k in range(1, N):
            rs_copy(g, k).wait_send()
            ag_copy(g, k).wait_send()
        return 0

    lax.fori_loop(0, GROUPS, sent, 0)
    for k in range(1, N):
        rs2_copy(k).wait_send()
        ag2_copy(k).wait_send()


def turns():
    half = HEAD // 2
    angle = (CACHE - 1) * np.float64(THETA) ** (-np.arange(half) / half)
    table = np.stack([np.cos(angle), np.sin(angle)]).astype(np.float32)
    return np.tile(table, (1, 2 * HEADS))


def solution(mesh):
    dma = pltpu.SemaphoreType.DMA

    def step(x, k_cache, v_cache, gain_a, wq, wo, gain_m, w_gate, w_up, w_down):
        k = k_cache.transpose(0, 2, 3, 1).reshape(CHUNKS, SEQS * QD, CACHE)
        v = v_cache.transpose(0, 2, 3, 1).reshape(CHUNKS, SEQS * QD, CACHE)
        vm = pltpu.VMEM
        return pl.pallas_call(
            kernel,
            out_shape=jax.ShapeDtypeStruct((ROWS, D), BF16),
            in_specs=[pl.BlockSpec(memory_space=pl.ANY)] * 11,
            out_specs=pl.BlockSpec(memory_space=pl.ANY),
            scratch_shapes=[
                vm((ROWS, D), BF16), vm((1, D), BF16), vm((1, D), BF16), vm((2, QD), F32),
                vm((D, QD), BF16), vm((QD, D), BF16), vm((D, FF), BF16), vm((D, FF), BF16), vm((FF, D), BF16),
                vm((SLOTS, SEQS * QD, CACHE), BF16), vm((SLOTS, SEQS * QD, CACHE), BF16),
                vm((ROWS, D), BF16), vm((ROWS, QD), F32), vm((SEQS * HEADS, CACHE), BF16), vm((ROWS, QD), F32),
                vm((GROUPS, N, GROUP, COLS), F32), vm((GROUPS, N, GROUP, COLS), BF16), vm((GROUPS, N, GROUP, COLS), BF16),
                vm((N, ROWS, COLS), BF16), vm((ROWS, FF), BF16),
                vm((N, ROWS, COLS), BF16), vm((N, ROWS, COLS), BF16), vm((N, ROWS, COLS), BF16),
                dma((7,)), dma((SLOTS,)), dma((SLOTS,)), dma((2, FF // MTILE)), dma((N,)),
                dma((GROUPS, N)), dma((GROUPS, N)), dma((GROUPS, N)), dma((GROUPS, N)),
                dma((N,)), dma((N,)), dma((N,)), dma((N,)),
            ],
            compiler_params=pltpu.CompilerParams(collective_id=0, has_side_effects=True, vmem_limit_bytes=66_000_000),
            name="layer",
        )(x, k, v, gain_a.reshape(1, D), wq, wo, gain_m.reshape(1, D), w_gate, w_up, w_down, jnp.asarray(turns()))

    states, cache, columns, rows_of = P("dp", None), P("dp", None, "tp", None), P(None, "tp"), P("tp", None)
    return jax.shard_map(
        step,
        mesh=mesh,
        in_specs=(states, cache, cache, P(None), columns, rows_of, P(None), columns, columns, rows_of),
        out_specs=states,
        check_vma=False,
    )
```

```python
import functools

import jax
import jax.numpy as jnp
import numpy as np
from jax import lax
from jax.experimental import pallas as pl
from jax.experimental.pallas import tpu as pltpu
from jax.sharding import PartitionSpec as P

HEAD = 96
THETA = 10000
N = 8
CHIPS = N // 2
ROWS, D = 64, 3072
COLS = D // N
HEADS = 4
QD = HEADS * HEAD
CACHE = 1024
FF = 1024
SEQS = 4
CHUNKS = ROWS // SEQS
SLOTS = 4
GROUP = 16
GROUPS = ROWS // GROUP
EARLY = GROUPS - 1
HALF = GROUP // 2
PER = GROUP // SEQS
MTILE = 256
PARTS = 2
PART = ROWS // PARTS
F32, BF16 = jnp.float32, jnp.bfloat16


def dot(a, b):
    return jnp.dot(a, b, preferred_element_type=F32)


def gain_of(ref, start, size):
    rows = range(start // 128, (start + size) // 128)
    return jnp.concatenate([ref[i:i + 1, :].astype(F32) for i in rows], 1)


def kernel(x_h, k_h, v_h, ga_h, wq_h, wo_h, gm_h, wg_h, wu_h, wd_h, cs_h, out_h,
           x_v, ga_v, gm_v, cs_v, wq_v, wo_v, wg_v, wu_v, wd_v, k_v, v_v,
           a_v, q_s, p_s, seen_s, term_s, tsend, trecv, psend, precv, chips, h_v, hid_v,
           ysend, yrecv, yown, ysum, yfar, y_v,
           in_sem, k_sem, v_sem, w_sem, rs_s, rs_r, ag_s, ag_r, pair_s, pair_r, chip_s, chip_r,
           in2_s, in2_r, rs2_s, rs2_r, ag2_s, ag2_r, out2_s, out2_r):
    me = lax.axis_index("tp")

    z, core = me // 2, lax.rem(me, 2)
    partner = 2 * z + 1 - core

    def peer(k):
        return lax.rem(me + k, N)

    def chip(k):
        return lax.rem(z + k, CHIPS)

    def remote(src, dst, send_sem, recv_sem, target):
        return pltpu.make_async_remote_copy(
            src_ref=src, dst_ref=dst, send_sem=send_sem, recv_sem=recv_sem,
            device_id={"tp": target}, device_id_type=pl.DeviceIdType.MESH)

    def local(src, dst, sem):
        return pltpu.make_async_copy(src, dst, sem)

    x_in = local(x_h, x_v, in_sem.at[0])
    ga_in = local(ga_h, ga_v, in_sem.at[1])
    cs_in = local(cs_h, cs_v, in_sem.at[2])
    wq_in = local(wq_h, wq_v, in_sem.at[3])
    wo_in = local(wo_h, wo_v, in_sem.at[4])
    gm_in = local(gm_h, gm_v, in_sem.at[5])

    def k_in(c):
        s = lax.rem(c, SLOTS)
        return local(k_h.at[c], k_v.at[s], k_sem.at[s])

    def v_in(c):
        s = lax.rem(c, SLOTS)
        return local(v_h.at[c], v_v.at[s], v_sem.at[s])

    def w_in(n):
        cols = pl.ds(n * MTILE, MTILE)
        return (local(wg_h.at[:, cols], wg_v.at[:, cols], w_sem.at[0, n]),
                local(wu_h.at[:, cols], wu_v.at[:, cols], w_sem.at[1, n]))

    wd_in = local(wd_h, wd_v, in_sem.at[6])

    x_in.start()
    ga_in.start()
    cs_in.start()
    wq_in.start()
    for c in range(SLOTS):
        k_in(c).start()
        v_in(c).start()
        if c == 0:
            wo_in.start()
            gm_in.start()

    barrier = pltpu.get_barrier_semaphore()
    for k in range(1, N):
        pl.semaphore_signal(barrier, inc=1, device_id={"tp": peer(k)}, device_id_type=pl.DeviceIdType.MESH)
    pl.semaphore_wait(barrier, N - 1)

    x_in.wait()
    ga_in.wait()

    def norm_x(i, _):
        rows = pl.ds(pl.multiple_of(i * GROUP, GROUP), GROUP)
        wide = x_v[rows, :].astype(F32)
        scale = lax.rsqrt(jnp.mean(wide * wide, -1, keepdims=True) + 1e-6)
        a_v[rows, :] = (wide * scale * gain_of(ga_v, 0, D)).astype(BF16)
        return 0

    lax.fori_loop(0, GROUPS, norm_x, 0)
    wq_in.wait()
    cs_in.wait()
    q = dot(a_v[...], wq_v[...]).astype(BF16).astype(F32)
    lane = lax.broadcasted_iota(jnp.int32, (ROWS, QD), 1)
    ahead = pltpu.roll(q, QD - HEAD // 2, 1)
    behind = pltpu.roll(q, HEAD // 2, 1)
    turn = jnp.where(lax.rem(lane, HEAD) < HEAD // 2, -ahead, behind)
    q_s[...] = (q * cs_v[0:1, :] + turn * cs_v[1:2, :]).astype(BF16).astype(F32)

    row16 = lax.broadcasted_iota(jnp.int32, (SEQS * HEADS, QD), 0)
    lane16 = lax.broadcasted_iota(jnp.int32, (SEQS * HEADS, QD), 1)
    masks = [row16 == i * HEADS + lane16 // HEAD for i in range(SEQS)]

    def weights_of(c):
        k_in(c).wait()
        parts = []
        for i in range(SEQS):
            row = q_s[pl.ds(c * SEQS + i, 1), :]
            parts.append(jnp.where(masks[i], jnp.broadcast_to(row, (SEQS * HEADS, QD)), 0.0))
        qd = jnp.concatenate(parts, 1).astype(BF16)
        s = dot(qd, k_v[lax.rem(c, SLOTS)]) * HEAD**-0.5
        e = jnp.exp(s - jnp.max(s, -1, keepdims=True))
        return (e * (1.0 / jnp.sum(e, -1, keepdims=True))).astype(BF16)

    def values_of(c, p):
        o = lax.dot_general(p, v_v[lax.rem(c, SLOTS)], (((1,), (1,)), ((), ())), preferred_element_type=F32)
        for i in range(SEQS):
            part = jnp.where(masks[i], o[:, i * QD:(i + 1) * QD], 0.0)
            seen_s[pl.ds(c * SEQS + i, 1), :] = jnp.sum(part, 0, keepdims=True)

    def group_rows(g):
        return pl.ds(pl.multiple_of(g * GROUP, GROUP), GROUP)

    def rs_copy(g, k):
        return remote(tsend.at[g, peer(k)], trecv.at[g, k], rs_s.at[g, k], rs_r.at[g, k], peer(k))

    def ag_copy(g, k):
        block = h_v.at[me, group_rows(g), :]
        return remote(block, block, ag_s.at[g, k], ag_r.at[g, k], peer(k))

    def send_terms(g):
        seen = seen_s[group_rows(g), :].astype(BF16)
        term = dot(seen, wo_v[...])
        for j in range(N):
            block = term[:, j * COLS:(j + 1) * COLS]
            term_s[g, j] = block
            tsend[g, j] = block.astype(BF16)
        for k in range(1, N):
            rs_copy(g, k).start()

    def finish_h(g):
        rows = group_rows(g)
        total = term_s[g, me]
        for k in range(1, N):
            rs_copy(g, k).wait_recv()
            total = total + trecv[g, k].astype(F32)
        mine = x_v[rows, pl.ds(pl.multiple_of(me * COLS, COLS), COLS)].astype(F32)
        h_v[me, rows, :] = (mine + total).astype(BF16)
        for k in range(1, N):
            ag_copy(g, k).start()

    def norm_h(rows):
        wide = [h_v[j, rows, :].astype(F32) for j in range(N)]
        square = sum(jnp.sum(w * w, -1, keepdims=True) for w in wide)
        scale = lax.rsqrt(square / D + 1e-6)
        for j in range(N):
            cols = slice(j * COLS, (j + 1) * COLS)
            a_v[rows, cols] = (wide[j] * scale * gain_of(gm_v, j * COLS, COLS)).astype(BF16)

    def early_h(g, _):
        for k in range(1, N):
            ag_copy(g, k).wait_recv()
        norm_h(group_rows(g))
        return 0

    def pair_copy(t):
        return remote(psend.at[t], precv.at[t], pair_s.at[t], pair_r.at[t], partner)

    def chip_copy(t, k, to, source):
        part = pl.ds(source * CHIPS, CHIPS)
        return remote(chips.at[t, 0, part], chips.at[t, k, part], chip_s.at[t, k, to], chip_r.at[t, k, source], 2 * chip(k) + to)

    def late_rows(t):
        return pl.ds(EARLY * GROUP + t * HALF, HALF)

    def send_pair(t):
        term = dot(seen_s[late_rows(t), :].astype(BF16), wo_v[...])
        for j in range(N):
            psend[t, j] = term[:, j * COLS:(j + 1) * COLS].astype(BF16)
        pair_copy(t).start()

    def send_chip(t):
        pair_copy(t).wait_recv()
        chips[t, 0] = (psend[t].astype(F32) + precv[t].astype(F32)).astype(BF16)
        for k in (2, 1, 3):
            for to in range(2):
                chip_copy(t, k, to, core).start()

    def late_h(t):
        for k in range(1, CHIPS):
            for source in range(2):
                chip_copy(t, k, 0, source).wait_recv()
        for j in range(N):
            total = x_v[late_rows(t), j * COLS:(j + 1) * COLS].astype(F32)
            for q in range(CHIPS):
                total = total + chips[t, lax.rem(z - q + CHIPS, CHIPS), j].astype(F32)
            h_v[j, late_rows(t), :] = total.astype(BF16)

    p_s[...] = weights_of(0)
    wo_in.wait()
    gm_in.wait()

    def chunk(c, _):
        @pl.when(c + SLOTS - 1 < CHUNKS)
        def _():
            k_in(c + SLOTS - 1).start()

        @pl.when(jnp.logical_and(c >= 2, c + SLOTS - 2 < CHUNKS))
        def _():
            v_in(c + SLOTS - 2).start()

        @pl.when(c == CHUNKS - SLOTS + 1)
        def _():
            for n in range(FF // MTILE):
                for w in w_in(n):
                    w.start()
            wd_in.start()

        v_in(c - 1).wait()
        p = p_s[...]
        p_s[...] = weights_of(c)
        values_of(c - 1, p)

        @pl.when(lax.rem(c, PER) == 0)
        def _():
            send_terms(c // PER - 1)

        @pl.when(c == CHUNKS - 2)
        def _():
            send_pair(0)

        @pl.when(c == CHUNKS - 1)
        def _():
            send_chip(0)

        @pl.when(jnp.logical_and(lax.rem(c, PER) == PER - 1, c >= 2 * PER - 1))
        def _():
            finish_h(c // PER - 1)

        return 0

    lax.fori_loop(1, CHUNKS, chunk, 0)
    v_in(CHUNKS - 1).wait()
    values_of(CHUNKS - 1, p_s[...])
    send_pair(1)
    late_h(0)
    send_chip(1)
    lax.fori_loop(0, EARLY, early_h, 0)
    late_h(1)
    norm_h(group_rows(EARLY))

    def hidden(n, _):
        for w in w_in(n):
            w.wait()
        cols = pl.ds(pl.multiple_of(n * MTILE, MTILE), MTILE)
        gate = dot(a_v[...], wg_v[:, cols])
        up = dot(a_v[...], wu_v[:, cols])
        hid_v[:, cols] = (jax.nn.silu(gate) * up).astype(BF16)
        return 0

    lax.fori_loop(0, FF // MTILE, hidden, 0)
    wd_in.wait()

    def in2(q):
        return remote(ysend.at[q], yrecv.at[q], in2_s.at[q], in2_r.at[q], partner)

    def part_rows(r):
        return pl.ds(r * PART, PART)

    def rs2(r, k):
        return remote(ysum.at[chip(k), part_rows(r)], yfar.at[k, part_rows(r)], rs2_s.at[r, k], rs2_r.at[r, k], 2 * chip(k) + core)

    mine = core * CHIPS + z

    def ag2(r, k, block):
        b = y_v.at[block, part_rows(r)]
        return remote(b, b, ag2_s.at[r, k], ag2_r.at[r, k], partner if k == 0 else 2 * chip(k) + core)

    def out2(r, k, block):
        b = y_v.at[block, part_rows(r)]
        return remote(b, b, out2_s.at[r, k], out2_r.at[r, k], partner)

    def down(half):
        return dot(hid_v[...], wd_v[:, pl.ds(pl.multiple_of(half * CHIPS * COLS, CHIPS * COLS), CHIPS * COLS)])

    theirs = down(1 - core)
    for q in range(CHIPS):
        ysend[q] = theirs[:, q * COLS:(q + 1) * COLS].astype(BF16)
    for k in (2, 1, 3, 0):
        in2(chip(k)).start()
    ours = down(core)
    for q in range(CHIPS):
        yown[q] = ours[:, q * COLS:(q + 1) * COLS]
    for k in (2, 1, 3):
        q = chip(k)
        in2(q).wait_recv()
        ysum[q] = (yown[q] + yrecv[q].astype(F32)).astype(BF16)
        rs2(0, k).start()
    for r in range(1, PARTS):
        for k in (2, 1, 3):
            rs2(r, k).start()
    in2(z).wait_recv()
    for r in range(PARTS):
        rows = part_rows(r)
        total = yown[z, rows, :] + yrecv[z, rows, :].astype(F32)
        for k in range(1, CHIPS):
            rs2(r, k).wait_recv()
            total = total + yfar[k, rows, :].astype(F32)
        y_v[mine, rows, :] = (h_v[mine, rows, :].astype(F32) + total).astype(BF16)
        for k in (2, 1, 3, 0):
            ag2(r, k, mine).start()
    for r in range(PARTS):
        for k in (1, 3, 2):
            block = core * CHIPS + chip(CHIPS - k)
            ag2(r, k, block).wait_recv()
            out2(r, k, block).start()
    for r in range(PARTS):
        ag2(r, 0, mine).wait_recv()
        for k in range(1, CHIPS):
            out2(r, k, mine).wait_recv()
    for j in range(N):
        out_h[:, j * COLS:(j + 1) * COLS] = y_v[j]

    def sent(g, _):
        for k in range(1, N):
            rs_copy(g, k).wait_send()
            ag_copy(g, k).wait_send()
        return 0

    lax.fori_loop(0, EARLY, sent, 0)
    for t in range(2):
        pair_copy(t).wait_send()
        for k in range(1, CHIPS):
            for to in range(2):
                chip_copy(t, k, to, core).wait_send()
    for q in range(CHIPS):
        in2(q).wait_send()
    for r in range(PARTS):
        ag2(r, 0, mine).wait_send()
        for k in range(1, CHIPS):
            rs2(r, k).wait_send()
            ag2(r, k, mine).wait_send()
            out2(r, k, mine).wait_send()


def turns():
    half = HEAD // 2
    angle = (CACHE - 1) * np.float64(THETA) ** (-np.arange(half) / half)
    table = np.stack([np.cos(angle), np.sin(angle)]).astype(np.float32)
    return np.tile(table, (1, 2 * HEADS))


def solution(mesh):
    dma = pltpu.SemaphoreType.DMA

    def step(x, k_cache, v_cache, gain_a, wq, wo, gain_m, w_gate, w_up, w_down):
        k = k_cache.transpose(0, 2, 3, 1).reshape(CHUNKS, SEQS * QD, CACHE)
        v = v_cache.transpose(0, 2, 3, 1).reshape(CHUNKS, SEQS * QD, CACHE)
        vm = pltpu.VMEM
        return pl.pallas_call(
            kernel,
            out_shape=pltpu.VMEM((ROWS, D), BF16),
            in_specs=[pl.BlockSpec(memory_space=pl.ANY)] * 11,
            out_specs=pl.BlockSpec(memory_space=pltpu.VMEM),
            scratch_shapes=[
                vm((ROWS, D), BF16), vm((24, 128), BF16), vm((24, 128), BF16), vm((2, QD), F32),
                vm((D, QD), BF16), vm((QD, D), BF16), vm((D, FF), BF16), vm((D, FF), BF16), vm((FF, D), BF16),
                vm((SLOTS, SEQS * QD, CACHE), BF16), vm((SLOTS, SEQS * QD, CACHE), BF16),
                vm((ROWS, D), BF16), vm((ROWS, QD), F32), vm((SEQS * HEADS, CACHE), BF16), vm((ROWS, QD), F32),
                vm((EARLY, N, GROUP, COLS), F32), vm((EARLY, N, GROUP, COLS), BF16), vm((EARLY, N, GROUP, COLS), BF16),
                vm((2, N, HALF, COLS), BF16), vm((2, N, HALF, COLS), BF16), vm((2, CHIPS, N, HALF, COLS), BF16),
                vm((N, ROWS, COLS), BF16), vm((ROWS, FF), BF16),
                vm((CHIPS, ROWS, COLS), BF16), vm((CHIPS, ROWS, COLS), BF16), vm((CHIPS, ROWS, COLS), F32),
                vm((CHIPS, ROWS, COLS), BF16), vm((CHIPS, ROWS, COLS), BF16), vm((N, ROWS, COLS), BF16),
                dma((7,)), dma((SLOTS,)), dma((SLOTS,)), dma((2, FF // MTILE)),
                dma((EARLY, N)), dma((EARLY, N)), dma((EARLY, N)), dma((EARLY, N)),
                dma((2,)), dma((2,)), dma((2, CHIPS, 2)), dma((2, CHIPS, 2)),
                dma((CHIPS,)), dma((CHIPS,)), dma((PARTS, CHIPS)), dma((PARTS, CHIPS)),
                dma((PARTS, CHIPS)), dma((PARTS, CHIPS)), dma((PARTS, CHIPS)), dma((PARTS, CHIPS)),
            ],
            compiler_params=pltpu.CompilerParams(collective_id=0, has_side_effects=True, vmem_limit_bytes=58_000_000),
            name="layer",
        )(x, k, v, gain_a.reshape(24, 128), wq, wo, gain_m.reshape(24, 128), w_gate, w_up, w_down, jnp.asarray(turns()))

    states, cache, columns, rows_of = P("dp", None), P("dp", None, "tp", None), P(None, "tp"), P("tp", None)
    return jax.shard_map(
        step,
        mesh=mesh,
        in_specs=(states, cache, cache, P(None), columns, rows_of, P(None), columns, columns, rows_of),
        out_specs=states,
        check_vma=False,
    )
```

```python
import functools

import jax
import jax.numpy as jnp
import numpy as np
from jax import lax
from jax.experimental import pallas as pl
from jax.experimental.pallas import tpu as pltpu
from jax.sharding import PartitionSpec as P

HEAD = 96
THETA = 10000
N = 8
CHIPS = N // 2
ROWS, D = 64, 3072
COLS = D // N
HEADS = 4
QD = HEADS * HEAD
CACHE = 1024
FF = 1024
SEQS = 4
CHUNKS = ROWS // SEQS
SLOTS = 4
GROUP = 16
GROUPS = ROWS // GROUP
EARLY = GROUPS - 1
HALF = GROUP // 2
PER = GROUP // SEQS
MTILE = 256
PART = 16
PARTS = EARLY * GROUP // PART
F32, BF16 = jnp.float32, jnp.bfloat16


def dot(a, b):
    return jnp.dot(a, b, preferred_element_type=F32)


def gain_of(ref, start, size):
    rows = range(start // 128, (start + size) // 128)
    return jnp.concatenate([ref[i:i + 1, :].astype(F32) for i in rows], 1)


def kernel(x_h, k_h, v_h, ga_h, wq_h, wo_h, gm_h, wg_h, wu_h, wd_h, cs_h, out_h,
           x_v, ga_v, gm_v, cs_v, wq_v, wo_v, wg_v, wu_v, wd_v, k_v, v_v,
           a_v, q_s, p_s, seen_s, term_s, tsend, trecv, psend, precv, chips, h_v, hid_v,
           ysend, yrecv, yown, ysum, yfar, y_v, zown, zsend, zrecv,
           in_sem, k_sem, v_sem, w_sem, rs_s, rs_r, ag_s, ag_r, pair_s, pair_r, chip_s, chip_r,
           in2_s, in2_r, rs2_s, rs2_r, ag2_s, ag2_r, out2_s, out2_r, rs3_s, rs3_r, ag3_s, ag3_r):
    me = lax.axis_index("tp")

    z, core = me // 2, lax.rem(me, 2)
    partner = 2 * z + 1 - core

    def peer(k):
        return lax.rem(me + k, N)

    def chip(k):
        return lax.rem(z + k, CHIPS)

    def remote(src, dst, send_sem, recv_sem, target):
        return pltpu.make_async_remote_copy(
            src_ref=src, dst_ref=dst, send_sem=send_sem, recv_sem=recv_sem,
            device_id={"tp": target}, device_id_type=pl.DeviceIdType.MESH)

    def local(src, dst, sem):
        return pltpu.make_async_copy(src, dst, sem)

    x_in = local(x_h, x_v, in_sem.at[0])
    ga_in = local(ga_h, ga_v, in_sem.at[1])
    cs_in = local(cs_h, cs_v, in_sem.at[2])
    wq_in = local(wq_h, wq_v, in_sem.at[3])
    wo_in = local(wo_h, wo_v, in_sem.at[4])
    gm_in = local(gm_h, gm_v, in_sem.at[5])

    def k_in(c):
        s = lax.rem(c, SLOTS)
        return local(k_h.at[c], k_v.at[s], k_sem.at[s])

    def v_in(c):
        s = lax.rem(c, SLOTS)
        return local(v_h.at[c], v_v.at[s], v_sem.at[s])

    def w_in(n):
        cols = pl.ds(n * MTILE, MTILE)
        return (local(wg_h.at[:, cols], wg_v.at[:, cols], w_sem.at[0, n]),
                local(wu_h.at[:, cols], wu_v.at[:, cols], w_sem.at[1, n]))

    wd_in = local(wd_h, wd_v, in_sem.at[6])

    x_in.start()
    ga_in.start()
    cs_in.start()
    wq_in.start()
    for c in range(SLOTS):
        k_in(c).start()
        v_in(c).start()
        if c == 0:
            wo_in.start()
            gm_in.start()

    barrier = pltpu.get_barrier_semaphore()
    for k in range(1, N):
        pl.semaphore_signal(barrier, inc=1, device_id={"tp": peer(k)}, device_id_type=pl.DeviceIdType.MESH)
    pl.semaphore_wait(barrier, N - 1)

    x_in.wait()
    ga_in.wait()

    def norm_x(i, _):
        rows = pl.ds(pl.multiple_of(i * GROUP, GROUP), GROUP)
        wide = x_v[rows, :].astype(F32)
        scale = lax.rsqrt(jnp.mean(wide * wide, -1, keepdims=True) + 1e-6)
        a_v[rows, :] = (wide * scale * gain_of(ga_v, 0, D)).astype(BF16)
        return 0

    lax.fori_loop(0, GROUPS, norm_x, 0)
    wq_in.wait()
    cs_in.wait()
    q = dot(a_v[...], wq_v[...]).astype(BF16).astype(F32)
    lane = lax.broadcasted_iota(jnp.int32, (ROWS, QD), 1)
    ahead = pltpu.roll(q, QD - HEAD // 2, 1)
    behind = pltpu.roll(q, HEAD // 2, 1)
    turn = jnp.where(lax.rem(lane, HEAD) < HEAD // 2, -ahead, behind)
    q_s[...] = (q * cs_v[0:1, :] + turn * cs_v[1:2, :]).astype(BF16).astype(F32)

    row16 = lax.broadcasted_iota(jnp.int32, (SEQS * HEADS, QD), 0)
    lane16 = lax.broadcasted_iota(jnp.int32, (SEQS * HEADS, QD), 1)
    masks = [row16 == i * HEADS + lane16 // HEAD for i in range(SEQS)]

    def weights_of(c):
        k_in(c).wait()
        parts = []
        for i in range(SEQS):
            row = q_s[pl.ds(c * SEQS + i, 1), :]
            parts.append(jnp.where(masks[i], jnp.broadcast_to(row, (SEQS * HEADS, QD)), 0.0))
        qd = jnp.concatenate(parts, 1).astype(BF16)
        s = dot(qd, k_v[lax.rem(c, SLOTS)]) * HEAD**-0.5
        e = jnp.exp(s - jnp.max(s, -1, keepdims=True))
        return (e * (1.0 / jnp.sum(e, -1, keepdims=True))).astype(BF16)

    def values_of(c, p):
        o = lax.dot_general(p, v_v[lax.rem(c, SLOTS)], (((1,), (1,)), ((), ())), preferred_element_type=F32)
        for i in range(SEQS):
            part = jnp.where(masks[i], o[:, i * QD:(i + 1) * QD], 0.0)
            seen_s[pl.ds(c * SEQS + i, 1), :] = jnp.sum(part, 0, keepdims=True)

    def group_rows(g):
        return pl.ds(pl.multiple_of(g * GROUP, GROUP), GROUP)

    def rs_copy(g, k, size=GROUP):
        part = pl.ds(0, size)
        return remote(tsend.at[g, peer(k), part], trecv.at[g, k, part], rs_s.at[g, k], rs_r.at[g, k], peer(k))

    def ag_copy(g, k, rows):
        block = h_v.at[me, rows, :]
        return remote(block, block, ag_s.at[g, k], ag_r.at[g, k], peer(k))

    FIRST, LAST = (pl.ds(EARLY * GROUP + t * HALF, HALF) for t in range(2))

    def send_terms(g, rows, size):
        term = dot(seen_s[rows, :].astype(BF16), wo_v[...])
        for j in range(N):
            block = term[:, j * COLS:(j + 1) * COLS]
            term_s[g, j, :size] = block
            tsend[g, j, :size] = block.astype(BF16)
        for k in range(1, N):
            rs_copy(g, k, size).start()

    def finish_h(g, rows, size):
        total = term_s[g, me, :size]
        for k in range(1, N):
            rs_copy(g, k, size).wait_recv()
            total = total + trecv[g, k, :size].astype(F32)
        mine = x_v[rows, pl.ds(pl.multiple_of(me * COLS, COLS), COLS)].astype(F32)
        h_v[me, rows, :] = (mine + total).astype(BF16)
        for k in range(1, N):
            ag_copy(g, k, rows).start()

    def norm_h(rows):
        wide = [h_v[j, rows, :].astype(F32) for j in range(N)]
        square = sum(jnp.sum(w * w, -1, keepdims=True) for w in wide)
        scale = lax.rsqrt(square / D + 1e-6)
        for j in range(N):
            cols = slice(j * COLS, (j + 1) * COLS)
            a_v[rows, cols] = (wide[j] * scale * gain_of(gm_v, j * COLS, COLS)).astype(BF16)

    def early_h(g, _):
        for k in range(1, N):
            ag_copy(g, k, group_rows(g)).wait_recv()
        norm_h(group_rows(g))
        return 0

    pair_copy = remote(psend, precv, pair_s, pair_r, partner)

    def chip_copy(k, to, source):
        part = pl.ds(source * CHIPS, CHIPS)
        return remote(chips.at[0, part], chips.at[k, part], chip_s.at[k, to], chip_r.at[k, source], 2 * chip(k) + to)

    def send_pair():
        term = dot(seen_s[LAST, :].astype(BF16), wo_v[...])
        for j in range(N):
            psend[j] = term[:, j * COLS:(j + 1) * COLS].astype(BF16)
        pair_copy.start()

    def send_chip():
        pair_copy.wait_recv()
        chips[0] = (psend[...].astype(F32) + precv[...].astype(F32)).astype(BF16)
        for k in (2, 1, 3):
            for to in range(2):
                chip_copy(k, to, core).start()

    def last_h():
        for k in range(1, CHIPS):
            for source in range(2):
                chip_copy(k, 0, source).wait_recv()
        for j in range(N):
            total = x_v[LAST, j * COLS:(j + 1) * COLS].astype(F32)
            for q in range(CHIPS):
                total = total + chips[lax.rem(z - q + CHIPS, CHIPS), j].astype(F32)
            h_v[j, LAST, :] = total.astype(BF16)

    p_s[...] = weights_of(0)
    wo_in.wait()
    gm_in.wait()

    def chunk(c, _):
        @pl.when(c + SLOTS - 1 < CHUNKS)
        def _():
            k_in(c + SLOTS - 1).start()

        @pl.when(jnp.logical_and(c >= 2, c + SLOTS - 2 < CHUNKS))
        def _():
            v_in(c + SLOTS - 2).start()

        @pl.when(c == CHUNKS - SLOTS + 1)
        def _():
            for n in range(FF // MTILE):
                for w in w_in(n):
                    w.start()
            wd_in.start()

        v_in(c - 1).wait()
        p = p_s[...]
        p_s[...] = weights_of(c)
        values_of(c - 1, p)

        @pl.when(lax.rem(c, PER) == 0)
        def _():
            send_terms(c // PER - 1, group_rows(c // PER - 1), GROUP)

        @pl.when(c == CHUNKS - 2)
        def _():
            send_terms(EARLY, FIRST, HALF)

        @pl.when(jnp.logical_and(lax.rem(c, PER) == 2, c >= PER + 2))
        def _():
            finish_h(c // PER - 1, group_rows(c // PER - 1), GROUP)

        return 0

    lax.fori_loop(1, CHUNKS, chunk, 0)
    v_in(CHUNKS - 1).wait()
    values_of(CHUNKS - 1, p_s[...])
    send_pair()
    finish_h(EARLY, FIRST, HALF)
    send_chip()
    lax.fori_loop(0, EARLY, early_h, 0)

    ONE, TWO = pl.ds(0, EARLY * GROUP), pl.ds(EARLY * GROUP, GROUP)

    def hidden(rows, n):
        cols = pl.ds(pl.multiple_of(n * MTILE, MTILE), MTILE)
        gate = dot(a_v[rows, :], wg_v[:, cols])
        up = dot(a_v[rows, :], wu_v[:, cols])
        hid_v[rows, cols] = (jax.nn.silu(gate) * up).astype(BF16)

    def hidden_one(n, _):
        for w in w_in(n):
            w.wait()
        hidden(ONE, n)
        return 0

    def hidden_two(n, _):
        hidden(TWO, n)
        return 0

    lax.fori_loop(0, FF // MTILE, hidden_one, 0)
    wd_in.wait()

    def in2(q):
        return remote(ysend.at[q], yrecv.at[q], in2_s.at[q], in2_r.at[q], partner)

    def part_rows(r):
        return pl.ds(r * PART, PART)

    def rs2(r, k):
        return remote(ysum.at[chip(k), part_rows(r)], yfar.at[k, part_rows(r)], rs2_s.at[r, k], rs2_r.at[r, k], 2 * chip(k) + core)

    mine = core * CHIPS + z

    def ag2(r, k, block):
        b = y_v.at[block, part_rows(r)]
        return remote(b, b, ag2_s.at[r, k], ag2_r.at[r, k], partner if k == 0 else 2 * chip(k) + core)

    def out2(r, k, block):
        b = y_v.at[block, part_rows(r)]
        return remote(b, b, out2_s.at[r, k], out2_r.at[r, k], partner)

    def down(half):
        return dot(hid_v[ONE, :], wd_v[:, pl.ds(pl.multiple_of(half * CHIPS * COLS, CHIPS * COLS), CHIPS * COLS)])

    def rs3(k):
        return remote(zsend.at[peer(k)], zrecv.at[k], rs3_s.at[k], rs3_r.at[k], peer(k))

    def ag3(k):
        b = y_v.at[me, TWO]
        return remote(b, b, ag3_s.at[k], ag3_r.at[k], peer(k))

    theirs = down(1 - core)
    for q in range(CHIPS):
        ysend[q] = theirs[:, q * COLS:(q + 1) * COLS].astype(BF16)
    for k in (2, 1, 3, 0):
        in2(chip(k)).start()
    ours = down(core)
    for q in range(CHIPS):
        yown[q] = ours[:, q * COLS:(q + 1) * COLS]
    for k in (2, 1, 3):
        q = chip(k)
        in2(q).wait_recv()
        ysum[q] = (yown[q] + yrecv[q].astype(F32)).astype(BF16)
    for r in range(PARTS):
        for k in (2, 1, 3):
            rs2(r, k).start()
    in2(z).wait_recv()

    for k in range(1, N):
        ag_copy(EARLY, k, FIRST).wait_recv()
    last_h()
    norm_h(TWO)
    lax.fori_loop(0, FF // MTILE, hidden_two, 0)
    last = dot(hid_v[TWO, :], wd_v[...])
    for j in range(N):
        block = last[:, j * COLS:(j + 1) * COLS]
        zown[j] = block
        zsend[j] = block.astype(BF16)
    for k in range(1, N):
        rs3(k).start()

    for r in range(PARTS):
        rows = part_rows(r)
        total = yown[z, rows, :] + yrecv[z, rows, :].astype(F32)
        for k in range(1, CHIPS):
            rs2(r, k).wait_recv()
            total = total + yfar[k, rows, :].astype(F32)
        y_v[mine, rows, :] = (h_v[mine, rows, :].astype(F32) + total).astype(BF16)
        for k in (2, 1, 3, 0):
            ag2(r, k, mine).start()
    total = zown[me]
    for k in range(1, N):
        rs3(k).wait_recv()
        total = total + zrecv[k].astype(F32)
    y_v[me, TWO, :] = (h_v[me, TWO, :].astype(F32) + total).astype(BF16)
    for k in range(1, N):
        ag3(k).start()
    for r in range(PARTS):
        for k in (1, 3, 2):
            block = core * CHIPS + chip(CHIPS - k)
            ag2(r, k, block).wait_recv()
            out2(r, k, block).start()
    for r in range(PARTS):
        ag2(r, 0, mine).wait_recv()
        for k in range(1, CHIPS):
            out2(r, k, mine).wait_recv()
    for k in range(1, N):
        ag3(k).wait_recv()
    for j in range(N):
        out_h[:, j * COLS:(j + 1) * COLS] = y_v[j]

    def sent(g, _):
        for k in range(1, N):
            rs_copy(g, k).wait_send()
            ag_copy(g, k, group_rows(g)).wait_send()
        return 0

    lax.fori_loop(0, EARLY, sent, 0)
    for k in range(1, N):
        rs_copy(EARLY, k, HALF).wait_send()
        ag_copy(EARLY, k, FIRST).wait_send()
        rs3(k).wait_send()
        ag3(k).wait_send()
    pair_copy.wait_send()
    for k in range(1, CHIPS):
        for to in range(2):
            chip_copy(k, to, core).wait_send()
    for q in range(CHIPS):
        in2(q).wait_send()
    for r in range(PARTS):
        ag2(r, 0, mine).wait_send()
        for k in range(1, CHIPS):
            rs2(r, k).wait_send()
            ag2(r, k, mine).wait_send()
            out2(r, k, mine).wait_send()


def turns():
    half = HEAD // 2
    angle = (CACHE - 1) * np.float64(THETA) ** (-np.arange(half) / half)
    table = np.stack([np.cos(angle), np.sin(angle)]).astype(np.float32)
    return np.tile(table, (1, 2 * HEADS))


def solution(mesh):
    dma = pltpu.SemaphoreType.DMA

    def step(x, k_cache, v_cache, gain_a, wq, wo, gain_m, w_gate, w_up, w_down):
        k = k_cache.transpose(0, 2, 3, 1).reshape(CHUNKS, SEQS * QD, CACHE)
        v = v_cache.transpose(0, 2, 3, 1).reshape(CHUNKS, SEQS * QD, CACHE)
        vm = pltpu.VMEM
        return pl.pallas_call(
            kernel,
            out_shape=pltpu.VMEM((ROWS, D), BF16),
            in_specs=[pl.BlockSpec(memory_space=pl.ANY)] * 11,
            out_specs=pl.BlockSpec(memory_space=pltpu.VMEM),
            scratch_shapes=[
                vm((ROWS, D), BF16), vm((24, 128), BF16), vm((24, 128), BF16), vm((2, QD), F32),
                vm((D, QD), BF16), vm((QD, D), BF16), vm((D, FF), BF16), vm((D, FF), BF16), vm((FF, D), BF16),
                vm((SLOTS, SEQS * QD, CACHE), BF16), vm((SLOTS, SEQS * QD, CACHE), BF16),
                vm((ROWS, D), BF16), vm((ROWS, QD), F32), vm((SEQS * HEADS, CACHE), BF16), vm((ROWS, QD), F32),
                vm((GROUPS, N, GROUP, COLS), F32), vm((GROUPS, N, GROUP, COLS), BF16), vm((GROUPS, N, GROUP, COLS), BF16),
                vm((N, HALF, COLS), BF16), vm((N, HALF, COLS), BF16), vm((CHIPS, N, HALF, COLS), BF16),
                vm((N, ROWS, COLS), BF16), vm((ROWS, FF), BF16),
                vm((CHIPS, EARLY * GROUP, COLS), BF16), vm((CHIPS, EARLY * GROUP, COLS), BF16), vm((CHIPS, EARLY * GROUP, COLS), F32),
                vm((CHIPS, EARLY * GROUP, COLS), BF16), vm((CHIPS, EARLY * GROUP, COLS), BF16), vm((N, ROWS, COLS), BF16),
                vm((N, GROUP, COLS), F32), vm((N, GROUP, COLS), BF16), vm((N, GROUP, COLS), BF16),
                dma((7,)), dma((SLOTS,)), dma((SLOTS,)), dma((2, FF // MTILE)),
                dma((GROUPS, N)), dma((GROUPS, N)), dma((GROUPS, N)), dma((GROUPS, N)),
                dma, dma, dma((CHIPS, 2)), dma((CHIPS, 2)),
                dma((CHIPS,)), dma((CHIPS,)), dma((PARTS, CHIPS)), dma((PARTS, CHIPS)),
                dma((PARTS, CHIPS)), dma((PARTS, CHIPS)), dma((PARTS, CHIPS)), dma((PARTS, CHIPS)),
                dma((N,)), dma((N,)), dma((N,)), dma((N,)),
            ],
            compiler_params=pltpu.CompilerParams(collective_id=0, has_side_effects=True, vmem_limit_bytes=58_000_000),
            name="layer",
        )(x, k, v, gain_a.reshape(24, 128), wq, wo, gain_m.reshape(24, 128), w_gate, w_up, w_down, jnp.asarray(turns()))

    states, cache, columns, rows_of = P("dp", None), P("dp", None, "tp", None), P(None, "tp"), P("tp", None)
    return jax.shard_map(
        step,
        mesh=mesh,
        in_specs=(states, cache, cache, P(None), columns, rows_of, P(None), columns, columns, rows_of),
        out_specs=states,
        check_vma=False,
    )
```

```python
import functools

import jax
import jax.numpy as jnp
import numpy as np
from jax import lax
from jax.experimental import pallas as pl
from jax.experimental.pallas import tpu as pltpu
from jax.sharding import PartitionSpec as P

HEAD = 96
THETA = 10000
N = 8
CHIPS = N // 2
ROWS, D = 64, 3072
COLS = D // N
HEADS = 4
QD = HEADS * HEAD
CACHE = 1024
FF = 1024
SEQS = 4
CHUNKS = ROWS // SEQS
SLOTS = 4
GROUP = 16
GROUPS = ROWS // GROUP
EARLY = GROUPS - 1
HALF = GROUP // 2
PER = GROUP // SEQS
MTILE = 256
PART = 16
PARTS = EARLY * GROUP // PART
F32, BF16 = jnp.float32, jnp.bfloat16


def dot(a, b):
    return jnp.dot(a, b, preferred_element_type=F32)


def gain_of(ref, start, size):
    rows = range(start // 128, (start + size) // 128)
    return jnp.concatenate([ref[i:i + 1, :].astype(F32) for i in rows], 1)


def kernel(x_h, k_h, v_h, ga_h, wq_h, wo_h, gm_h, wg_h, wu_h, wd_h, cs_h, out_h,
           x_v, ga_v, gm_v, cs_v, wq_v, wo_v, wg_v, wu_v, wd_v, k_v, v_v,
           a_v, q_s, p_s, seen_s, term_s, tsend, trecv, psend, precv, chips, h_v, hid_v,
           ysend, yrecv, yown, ysum, yfar, y_v, zown, zsend, zrecv,
           in_sem, k_sem, v_sem, w_sem, rs_s, rs_r, ag_s, ag_r, pair_s, pair_r, chip_s, chip_r,
           in2_s, in2_r, rs2_s, rs2_r, ag2_r, out2_s, out2_r, rs3_s, rs3_r, ag3_s, ag3_r):
    me = lax.axis_index("tp")

    z, core = me // 2, lax.rem(me, 2)
    partner = 2 * z + 1 - core

    def peer(k):
        return lax.rem(me + k, N)

    def chip(k):
        return lax.rem(z + k, CHIPS)

    def arrived(like, sem):
        pltpu.make_async_copy(like, like, sem).wait()

    def remote(src, dst, send_sem, recv_sem, target):
        return pltpu.make_async_remote_copy(
            src_ref=src, dst_ref=dst, send_sem=send_sem, recv_sem=recv_sem,
            device_id={"tp": target}, device_id_type=pl.DeviceIdType.MESH)

    def local(src, dst, sem):
        return pltpu.make_async_copy(src, dst, sem)

    x_in = local(x_h, x_v, in_sem.at[0])
    ga_in = local(ga_h, ga_v, in_sem.at[1])
    cs_in = local(cs_h, cs_v, in_sem.at[2])
    wq_in = local(wq_h, wq_v, in_sem.at[3])
    wo_in = local(wo_h, wo_v, in_sem.at[4])
    gm_in = local(gm_h, gm_v, in_sem.at[5])

    def k_in(c):
        s = lax.rem(c, SLOTS)
        return local(k_h.at[c], k_v.at[s], k_sem.at[s])

    def v_in(c):
        s = lax.rem(c, SLOTS)
        return local(v_h.at[c], v_v.at[s], v_sem.at[s])

    wg_in = local(wg_h, wg_v, w_sem.at[0])
    wu_in = local(wu_h, wu_v, w_sem.at[1])
    wd_in = local(wd_h, wd_v, w_sem.at[2])

    x_in.start()
    ga_in.start()
    cs_in.start()
    wq_in.start()
    for c in range(SLOTS):
        k_in(c).start()
        v_in(c).start()
        if c == 0:
            wo_in.start()
            gm_in.start()

    barrier = pltpu.get_barrier_semaphore()
    for k in range(1, N):
        pl.semaphore_signal(barrier, inc=1, device_id={"tp": peer(k)}, device_id_type=pl.DeviceIdType.MESH)

    x_in.wait()
    ga_in.wait()

    def norm_x(i, _):
        rows = pl.ds(pl.multiple_of(i * GROUP, GROUP), GROUP)
        wide = x_v[rows, :].astype(F32)
        scale = lax.rsqrt(jnp.mean(wide * wide, -1, keepdims=True) + 1e-6)
        a_v[rows, :] = (wide * scale * gain_of(ga_v, 0, D)).astype(BF16)
        return 0

    lax.fori_loop(0, GROUPS, norm_x, 0)
    wq_in.wait()
    cs_in.wait()
    q = dot(a_v[...], wq_v[...]).astype(BF16).astype(F32)
    lane = lax.broadcasted_iota(jnp.int32, (ROWS, QD), 1)
    ahead = pltpu.roll(q, QD - HEAD // 2, 1)
    behind = pltpu.roll(q, HEAD // 2, 1)
    turn = jnp.where(lax.rem(lane, HEAD) < HEAD // 2, -ahead, behind)
    q_s[...] = (q * cs_v[0:1, :] + turn * cs_v[1:2, :]).astype(BF16).astype(F32)

    row16 = lax.broadcasted_iota(jnp.int32, (SEQS * HEADS, QD), 0)
    lane16 = lax.broadcasted_iota(jnp.int32, (SEQS * HEADS, QD), 1)
    masks = [row16 == i * HEADS + lane16 // HEAD for i in range(SEQS)]

    def weights_of(c):
        k_in(c).wait()
        parts = []
        for i in range(SEQS):
            row = q_s[pl.ds(c * SEQS + i, 1), :]
            parts.append(jnp.where(masks[i], jnp.broadcast_to(row, (SEQS * HEADS, QD)), 0.0))
        qd = jnp.concatenate(parts, 1).astype(BF16)
        s = dot(qd, k_v[lax.rem(c, SLOTS)]) * HEAD**-0.5
        e = jnp.exp(s - jnp.max(s, -1, keepdims=True))
        return (e * (1.0 / jnp.sum(e, -1, keepdims=True))).astype(BF16)

    def values_of(c, p):
        o = lax.dot_general(p, v_v[lax.rem(c, SLOTS)], (((1,), (1,)), ((), ())), preferred_element_type=F32)
        for i in range(SEQS):
            part = jnp.where(masks[i], o[:, i * QD:(i + 1) * QD], 0.0)
            seen_s[pl.ds(c * SEQS + i, 1), :] = jnp.sum(part, 0, keepdims=True)

    def group_rows(g):
        return pl.ds(pl.multiple_of(g * GROUP, GROUP), GROUP)

    def rs_copy(g, k, size=GROUP):
        part = pl.ds(0, size)
        return remote(tsend.at[g, peer(k), part], trecv.at[g, k, part], rs_s.at[g], rs_r.at[g], peer(k))

    def ag_copy(g, k, rows):
        block = h_v.at[me, rows, :]
        return remote(block, block, ag_s.at[g], ag_r.at[g], peer(k))

    FIRST, LAST = (pl.ds(EARLY * GROUP + t * HALF, HALF) for t in range(2))

    def send_terms(g, rows, size):
        term = dot(seen_s[rows, :].astype(BF16), wo_v[...])
        for j in range(N):
            block = term[:, j * COLS:(j + 1) * COLS]
            term_s[g, j, :size] = block
            tsend[g, j, :size] = block.astype(BF16)
        for k in range(1, N):
            rs_copy(g, k, size).start()

    def finish_h(g, rows, size):
        arrived(trecv.at[g, pl.ds(1, N - 1), pl.ds(0, size)], rs_r.at[g])
        total = term_s[g, me, :size]
        for k in range(1, N):
            total = total + trecv[g, k, :size].astype(F32)
        mine = x_v[rows, pl.ds(pl.multiple_of(me * COLS, COLS), COLS)].astype(F32)
        h_v[me, rows, :] = (mine + total).astype(BF16)
        for k in range(1, N):
            ag_copy(g, k, rows).start()

    def norm_h(rows):
        wide = [h_v[j, rows, :].astype(F32) for j in range(N)]
        square = sum(jnp.sum(w * w, -1, keepdims=True) for w in wide)
        scale = lax.rsqrt(square / D + 1e-6)
        for j in range(N):
            cols = slice(j * COLS, (j + 1) * COLS)
            a_v[rows, cols] = (wide[j] * scale * gain_of(gm_v, j * COLS, COLS)).astype(BF16)

    def early_h(g, _):
        arrived(h_v.at[pl.ds(0, N - 1), group_rows(g)], ag_r.at[g])
        norm_h(group_rows(g))
        return 0

    pair_copy = remote(psend, precv, pair_s, pair_r, partner)

    def chip_copy(k, to):
        part = pl.ds(core * CHIPS, CHIPS)
        return remote(chips.at[0, part], chips.at[k, part], chip_s, chip_r, 2 * chip(k) + to)

    def send_pair():
        term = dot(seen_s[LAST, :].astype(BF16), wo_v[...])
        for j in range(N):
            psend[j] = term[:, j * COLS:(j + 1) * COLS].astype(BF16)
        pair_copy.start()

    def send_chip():
        pair_copy.wait_recv()
        chips[0] = (psend[...].astype(F32) + precv[...].astype(F32)).astype(BF16)
        for k in (2, 1, 3):
            for to in range(2):
                chip_copy(k, to).start()

    def last_h():
        arrived(chips.at[pl.ds(1, CHIPS - 1)], chip_r)
        for j in range(N):
            total = x_v[LAST, j * COLS:(j + 1) * COLS].astype(F32)
            for q in range(CHIPS):
                total = total + chips[lax.rem(z - q + CHIPS, CHIPS), j].astype(F32)
            h_v[j, LAST, :] = total.astype(BF16)

    p_s[...] = weights_of(0)
    def chunk(c, _):
        @pl.when(c + SLOTS - 1 < CHUNKS)
        def _():
            k_in(c + SLOTS - 1).start()

        @pl.when(jnp.logical_and(c >= 2, c + SLOTS - 2 < CHUNKS))
        def _():
            v_in(c + SLOTS - 2).start()

        @pl.when(c == CHUNKS - SLOTS + 1)
        def _():
            for w in (wg_in, wu_in, wd_in):
                w.start(priority=1)

        v_in(c - 1).wait()
        p = p_s[...]
        p_s[...] = weights_of(c)
        values_of(c - 1, p)

        @pl.when(c == PER)
        def _():
            pl.semaphore_wait(barrier, N - 1)
            wo_in.wait()
            gm_in.wait()

        @pl.when(lax.rem(c, PER) == 0)
        def _():
            send_terms(c // PER - 1, group_rows(c // PER - 1), GROUP)

        @pl.when(c == CHUNKS - 2)
        def _():
            send_terms(EARLY, FIRST, HALF)

        @pl.when(jnp.logical_and(lax.rem(c, PER) == 2, c >= PER + 2))
        def _():
            finish_h(c // PER - 1, group_rows(c // PER - 1), GROUP)

        return 0

    lax.fori_loop(1, CHUNKS, chunk, 0)
    v_in(CHUNKS - 1).wait()
    values_of(CHUNKS - 1, p_s[...])
    send_pair()
    finish_h(EARLY, FIRST, HALF)
    send_chip()
    lax.fori_loop(0, EARLY, early_h, 0)

    ONE, TWO = pl.ds(0, EARLY * GROUP), pl.ds(EARLY * GROUP, GROUP)

    def hidden(rows, n):
        cols = pl.ds(pl.multiple_of(n * MTILE, MTILE), MTILE)
        gate = dot(a_v[rows, :], wg_v[:, cols])
        up = dot(a_v[rows, :], wu_v[:, cols])
        hid_v[rows, cols] = (jax.nn.silu(gate) * up).astype(BF16)

    wg_in.wait()
    wu_in.wait()
    for n in range(FF // MTILE):
        hidden(ONE, n)
    wd_in.wait()

    in2 = remote(ysend, yrecv, in2_s, in2_r, partner)

    def part_rows(r):
        return pl.ds(r * PART, PART)

    def rs2(r, k):
        return remote(ysum.at[chip(k), part_rows(r)], yfar.at[k, part_rows(r)], rs2_s, rs2_r.at[r], 2 * chip(k) + core)

    mine = core * CHIPS + z

    def ag2(r, k):
        b = y_v.at[mine, part_rows(r)]
        return remote(b, b, out2_s, ag2_r.at[r], 2 * chip(k) + core)

    def out2(r, k):
        b = y_v.at[core * CHIPS + chip(CHIPS - k), part_rows(r)]
        return remote(b, b, out2_s, out2_r, partner)

    def down(half):
        return dot(hid_v[ONE, :], wd_v[:, pl.ds(pl.multiple_of(half * CHIPS * COLS, CHIPS * COLS), CHIPS * COLS)])

    def rs3(k):
        return remote(zsend.at[peer(k)], zrecv.at[k], rs3_s, rs3_r, peer(k))

    def ag3(k):
        b = y_v.at[me, TWO]
        return remote(b, b, ag3_s, ag3_r, peer(k))

    theirs = down(1 - core)
    for q in range(CHIPS):
        ysend[q] = theirs[:, q * COLS:(q + 1) * COLS].astype(BF16)
    in2.start()
    ours = down(core)
    for q in range(CHIPS):
        yown[q] = ours[:, q * COLS:(q + 1) * COLS]
    in2.wait_recv()
    for k in (2, 1, 3):
        q = chip(k)
        ysum[q] = (yown[q] + yrecv[q].astype(F32)).astype(BF16)
    for r in range(PARTS):
        for k in (2, 1, 3):
            rs2(r, k).start()

    arrived(h_v.at[pl.ds(0, N - 1), FIRST], ag_r.at[EARLY])
    last_h()
    norm_h(TWO)
    for n in range(FF // MTILE):
        hidden(TWO, n)
    last = dot(hid_v[TWO, :], wd_v[...])
    for j in range(N):
        block = last[:, j * COLS:(j + 1) * COLS]
        zown[j] = block
        zsend[j] = block.astype(BF16)
    for k in range(1, N):
        rs3(k).start()

    for r in range(PARTS):
        rows = part_rows(r)
        total = yown[z, rows, :] + yrecv[z, rows, :].astype(F32)
        arrived(yfar.at[pl.ds(1, CHIPS - 1), rows], rs2_r.at[r])
        for k in range(1, CHIPS):
            total = total + yfar[k, rows, :].astype(F32)
        y_v[mine, rows, :] = (h_v[mine, rows, :].astype(F32) + total).astype(BF16)
        for k in (2, 1, 3):
            ag2(r, k).start()
        out2(r, 0).start()
    arrived(zrecv.at[pl.ds(1, N - 1)], rs3_r)
    total = zown[me]
    for k in range(1, N):
        total = total + zrecv[k].astype(F32)
    y_v[me, TWO, :] = (h_v[me, TWO, :].astype(F32) + total).astype(BF16)
    for k in range(1, N):
        ag3(k).start()
    for r in range(PARTS):
        arrived(y_v.at[pl.ds(0, CHIPS - 1), part_rows(r)], ag2_r.at[r])
        for k in (1, 3, 2):
            out2(r, k).start()
    arrived(y_v.at[pl.ds(0, CHIPS), ONE], out2_r)
    arrived(y_v.at[pl.ds(0, N - 1), TWO], ag3_r)
    for j in range(N):
        out_h[:, j * COLS:(j + 1) * COLS] = y_v[j]

    for g in range(GROUPS):
        part = pl.ds(0, GROUP if g < EARLY else HALF)
        arrived(tsend.at[g, pl.ds(0, N - 1), part], rs_s.at[g])
        arrived(tsend.at[g, pl.ds(0, N - 1), part], ag_s.at[g])
    pair_copy.wait_send()
    arrived(chips.at[pl.ds(0, CHIPS - 1)], chip_s)
    in2.wait_send()
    arrived(ysum.at[pl.ds(0, CHIPS - 1)], rs2_s)
    arrived(y_v.at[pl.ds(0, N - 1), ONE], out2_s)
    arrived(zsend.at[pl.ds(0, N - 1)], rs3_s)
    arrived(zsend.at[pl.ds(0, N - 1)], ag3_s)


def turns():
    half = HEAD // 2
    angle = (CACHE - 1) * np.float64(THETA) ** (-np.arange(half) / half)
    table = np.stack([np.cos(angle), np.sin(angle)]).astype(np.float32)
    return np.tile(table, (1, 2 * HEADS))


def solution(mesh):
    dma = pltpu.SemaphoreType.DMA

    def step(x, k_cache, v_cache, gain_a, wq, wo, gain_m, w_gate, w_up, w_down):
        k = k_cache.transpose(0, 2, 3, 1).reshape(CHUNKS, SEQS * QD, CACHE)
        v = v_cache.transpose(0, 2, 3, 1).reshape(CHUNKS, SEQS * QD, CACHE)
        vm = pltpu.VMEM
        return pl.pallas_call(
            kernel,
            out_shape=pltpu.VMEM((ROWS, D), BF16),
            in_specs=[pl.BlockSpec(memory_space=pl.ANY)] * 11,
            out_specs=pl.BlockSpec(memory_space=pltpu.VMEM),
            scratch_shapes=[
                vm((ROWS, D), BF16), vm((24, 128), BF16), vm((24, 128), BF16), vm((2, QD), F32),
                vm((D, QD), BF16), vm((QD, D), BF16), vm((D, FF), BF16), vm((D, FF), BF16), vm((FF, D), BF16),
                vm((SLOTS, SEQS * QD, CACHE), BF16), vm((SLOTS, SEQS * QD, CACHE), BF16),
                vm((ROWS, D), BF16), vm((ROWS, QD), F32), vm((SEQS * HEADS, CACHE), BF16), vm((ROWS, QD), F32),
                vm((GROUPS, N, GROUP, COLS), F32), vm((GROUPS, N, GROUP, COLS), BF16), vm((GROUPS, N, GROUP, COLS), BF16),
                vm((N, HALF, COLS), BF16), vm((N, HALF, COLS), BF16), vm((CHIPS, N, HALF, COLS), BF16),
                vm((N, ROWS, COLS), BF16), vm((ROWS, FF), BF16),
                vm((CHIPS, EARLY * GROUP, COLS), BF16), vm((CHIPS, EARLY * GROUP, COLS), BF16), vm((CHIPS, EARLY * GROUP, COLS), F32),
                vm((CHIPS, EARLY * GROUP, COLS), BF16), vm((CHIPS, EARLY * GROUP, COLS), BF16), vm((N, ROWS, COLS), BF16),
                vm((N, GROUP, COLS), F32), vm((N, GROUP, COLS), BF16), vm((N, GROUP, COLS), BF16),
                dma((6,)), dma((SLOTS,)), dma((SLOTS,)), dma((3,)),
                dma((GROUPS,)), dma((GROUPS,)), dma((GROUPS,)), dma((GROUPS,)),
                dma, dma, dma, dma,
                dma, dma, dma, dma((PARTS,)), dma((PARTS,)), dma, dma, dma, dma, dma, dma,
            ],
            compiler_params=pltpu.CompilerParams(collective_id=0, has_side_effects=True, vmem_limit_bytes=58_000_000),
            name="layer",
        )(x, k, v, gain_a.reshape(24, 128), wq, wo, gain_m.reshape(24, 128), w_gate, w_up, w_down, jnp.asarray(turns()))

    states, cache, columns, rows_of = P("dp", None), P("dp", None, "tp", None), P(None, "tp"), P("tp", None)
    return jax.shard_map(
        step,
        mesh=mesh,
        in_specs=(states, cache, cache, P(None), columns, rows_of, P(None), columns, columns, rows_of),
        out_specs=states,
        check_vma=False,
    )
```

```python
import functools

import jax
import jax.numpy as jnp
import numpy as np
from jax import lax
from jax.experimental import pallas as pl
from jax.experimental.pallas import tpu as pltpu
from jax.sharding import PartitionSpec as P

HEAD = 96
THETA = 10000
N = 8
CHIPS = N // 2
ROWS, D = 64, 3072
COLS = D // N
HEADS = 4
QD = HEADS * HEAD
CACHE = 1024
FF = 1024
SEQS = 4
CHUNKS = ROWS // SEQS
SLOTS = 4
GROUP = 16
GROUPS = ROWS // GROUP
EARLY = GROUPS - 1
HALF = GROUP // 2
PER = GROUP // SEQS
MTILE = 256
PART = 16
PARTS = EARLY * GROUP // PART
F32, BF16 = jnp.float32, jnp.bfloat16


def dot(a, b):
    return jnp.dot(a, b, preferred_element_type=F32)


def gain_of(ref, start, size):
    rows = range(start // 128, (start + size) // 128)
    return jnp.concatenate([ref[i:i + 1, :].astype(F32) for i in rows], 1)


def kernel(x_h, k_h, v_h, ga_h, wq_h, wo_h, gm_h, wg_h, wu_h, wd_h, cs_h, out_h,
           x_v, ga_v, gm_v, cs_v, wq_v, wo_v, wg_v, wu_v, wd_v, k_v, v_v,
           a_v, q_s, p_s, seen_s, term_s, tsend, trecv, psend, precv, chips, h_v, hid_v,
           ysend, yrecv, yown, ysum, yfar, y_v, zown, zsend, zrecv,
           in_sem, k_sem, v_sem, w_sem, rs_s, rs_r, ag_s, ag_r, pair_s, pair_r, chip_s, chip_r, forward_s, forward_r,
           in2_s, in2_r, rs2_s, rs2_r, ag2_r, out2_s, out2_r, rs3_s, rs3_r, ag3_s, ag3_r, out3_r):
    me = lax.axis_index("tp")

    z, core = me // 2, lax.rem(me, 2)
    partner = 2 * z + 1 - core

    def peer(k):
        return lax.rem(me + k, N)

    def chip(k):
        return lax.rem(z + k, CHIPS)

    side = z // 2
    edge = z + side * (3 - 2 * z)
    others = [t + side * (3 - 2 * t) for t in (3, 2, 1 - edge)]
    devices = [2 * t + c for t in others for c in (core, 1 - core)] + [partner]

    def arrived(like, sem):
        pltpu.make_async_copy(like, like, sem).wait()

    def remote(src, dst, send_sem, recv_sem, target):
        return pltpu.make_async_remote_copy(
            src_ref=src, dst_ref=dst, send_sem=send_sem, recv_sem=recv_sem,
            device_id={"tp": target}, device_id_type=pl.DeviceIdType.MESH)

    def local(src, dst, sem):
        return pltpu.make_async_copy(src, dst, sem)

    x_in = local(x_h, x_v, in_sem.at[0])
    ga_in = local(ga_h, ga_v, in_sem.at[1])
    cs_in = local(cs_h, cs_v, in_sem.at[2])
    wq_in = local(wq_h, wq_v, in_sem.at[3])
    wo_in = local(wo_h, wo_v, in_sem.at[4])
    gm_in = local(gm_h, gm_v, in_sem.at[5])

    def k_in(c):
        s = lax.rem(c, SLOTS)
        return local(k_h.at[c], k_v.at[s], k_sem.at[s])

    def v_in(c):
        s = lax.rem(c, SLOTS)
        return local(v_h.at[c], v_v.at[s], v_sem.at[s])

    wg_in = local(wg_h, wg_v, w_sem.at[0])
    wu_in = local(wu_h, wu_v, w_sem.at[1])
    wd_in = local(wd_h, wd_v, w_sem.at[2])

    x_in.start()
    ga_in.start()
    cs_in.start()
    wq_in.start()
    for c in range(SLOTS):
        k_in(c).start()
        v_in(c).start()
        if c == 0:
            wo_in.start()
            gm_in.start()

    barrier = pltpu.get_barrier_semaphore()
    for k in range(1, N):
        pl.semaphore_signal(barrier, inc=1, device_id={"tp": peer(k)}, device_id_type=pl.DeviceIdType.MESH)

    x_in.wait()
    ga_in.wait()

    def norm_x(i, _):
        rows = pl.ds(pl.multiple_of(i * GROUP, GROUP), GROUP)
        wide = x_v[rows, :].astype(F32)
        scale = lax.rsqrt(jnp.mean(wide * wide, -1, keepdims=True) + 1e-6)
        a_v[rows, :] = (wide * scale * gain_of(ga_v, 0, D)).astype(BF16)
        return 0

    lax.fori_loop(0, GROUPS, norm_x, 0)
    wq_in.wait()
    cs_in.wait()
    q = dot(a_v[...], wq_v[...]).astype(BF16).astype(F32)
    lane = lax.broadcasted_iota(jnp.int32, (ROWS, QD), 1)
    ahead = pltpu.roll(q, QD - HEAD // 2, 1)
    behind = pltpu.roll(q, HEAD // 2, 1)
    turn = jnp.where(lax.rem(lane, HEAD) < HEAD // 2, -ahead, behind)
    q_s[...] = (q * cs_v[0:1, :] + turn * cs_v[1:2, :]).astype(BF16).astype(F32)

    row16 = lax.broadcasted_iota(jnp.int32, (SEQS * HEADS, QD), 0)
    lane16 = lax.broadcasted_iota(jnp.int32, (SEQS * HEADS, QD), 1)
    masks = [row16 == i * HEADS + lane16 // HEAD for i in range(SEQS)]

    def weights_of(c):
        k_in(c).wait()
        parts = []
        for i in range(SEQS):
            row = q_s[pl.ds(c * SEQS + i, 1), :]
            parts.append(jnp.where(masks[i], jnp.broadcast_to(row, (SEQS * HEADS, QD)), 0.0))
        qd = jnp.concatenate(parts, 1).astype(BF16)
        s = dot(qd, k_v[lax.rem(c, SLOTS)]) * HEAD**-0.5
        e = jnp.exp(s - jnp.max(s, -1, keepdims=True))
        return (e * (1.0 / jnp.sum(e, -1, keepdims=True))).astype(BF16)

    def values_of(c, p):
        o = lax.dot_general(p, v_v[lax.rem(c, SLOTS)], (((1,), (1,)), ((), ())), preferred_element_type=F32)
        for i in range(SEQS):
            part = jnp.where(masks[i], o[:, i * QD:(i + 1) * QD], 0.0)
            seen_s[pl.ds(c * SEQS + i, 1), :] = jnp.sum(part, 0, keepdims=True)

    def group_rows(g):
        return pl.ds(pl.multiple_of(g * GROUP, GROUP), GROUP)

    def rs_copy(g, to, size):
        part = pl.ds(0, size)
        return remote(tsend.at[g, to, part], trecv.at[g, me, part], rs_s.at[g], rs_r.at[g], to)

    def ag_copy(g, to, rows):
        block = h_v.at[me, rows, :]
        return remote(block, block, ag_s.at[g], ag_r.at[g], to)

    FIRST, LAST = (pl.ds(EARLY * GROUP + t * HALF, HALF) for t in range(2))

    def send_terms(g, rows, size):
        term = dot(seen_s[rows, :].astype(BF16), wo_v[...])
        for j in range(N):
            block = term[:, j * COLS:(j + 1) * COLS]
            term_s[g, j, :size] = block
            tsend[g, j, :size] = block.astype(BF16)
        for to in devices:
            rs_copy(g, to, size).start()

    def finish_h(g, rows, size):
        arrived(trecv.at[g, pl.ds(1, N - 1), pl.ds(0, size)], rs_r.at[g])
        total = term_s[g, me, :size]
        for k in range(1, N):
            total = total + trecv[g, peer(k), :size].astype(F32)
        mine = x_v[rows, pl.ds(pl.multiple_of(me * COLS, COLS), COLS)].astype(F32)
        h_v[me, rows, :] = (mine + total).astype(BF16)
        for to in devices:
            ag_copy(g, to, rows).start()

    def norm_h(rows):
        wide = [h_v[j, rows, :].astype(F32) for j in range(N)]
        square = sum(jnp.sum(w * w, -1, keepdims=True) for w in wide)
        scale = lax.rsqrt(square / D + 1e-6)
        for j in range(N):
            cols = slice(j * COLS, (j + 1) * COLS)
            a_v[rows, cols] = (wide[j] * scale * gain_of(gm_v, j * COLS, COLS)).astype(BF16)

    def early_h(g, _):
        arrived(h_v.at[pl.ds(0, N - 1), group_rows(g)], ag_r.at[g])
        norm_h(group_rows(g))
        return 0

    pair_copy = remote(psend, precv, pair_s, pair_r, partner)

    half = pl.ds(core * CHIPS, CHIPS)

    def chip_copy(to):
        return remote(chips.at[z, half], chips.at[z, half], chip_s, chip_r, 2 * to + core)

    def forward_copy(source):
        return remote(chips.at[source, half], chips.at[source, half], forward_s, forward_r, partner)

    def send_pair():
        term = dot(seen_s[LAST, :].astype(BF16), wo_v[...])
        for j in range(N):
            psend[j] = term[:, j * COLS:(j + 1) * COLS].astype(BF16)
        pair_copy.start()

    def send_chip():
        pair_copy.wait_recv()
        chips[z] = (psend[...].astype(F32) + precv[...].astype(F32)).astype(BF16)
        for to in others:
            chip_copy(to).start()

    def forward_chips():
        arrived(chips.at[pl.ds(0, CHIPS - 1), half], chip_r)
        for source in others:
            forward_copy(source).start()

    def last_h():
        arrived(chips.at[pl.ds(0, CHIPS - 1), half], forward_r)
        for j in range(N):
            total = x_v[LAST, j * COLS:(j + 1) * COLS].astype(F32)
            for q in range(CHIPS):
                total = total + chips[q, j].astype(F32)
            h_v[j, LAST, :] = total.astype(BF16)

    p_s[...] = weights_of(0)
    def chunk(c, _):
        @pl.when(c + SLOTS - 1 < CHUNKS)
        def _():
            k_in(c + SLOTS - 1).start()

        @pl.when(jnp.logical_and(c >= 2, c + SLOTS - 2 < CHUNKS))
        def _():
            v_in(c + SLOTS - 2).start()

        @pl.when(c == CHUNKS - SLOTS + 1)
        def _():
            for w in (wg_in, wu_in, wd_in):
                w.start(priority=1)

        v_in(c - 1).wait()
        p = p_s[...]
        p_s[...] = weights_of(c)
        values_of(c - 1, p)

        @pl.when(c == PER)
        def _():
            pl.semaphore_wait(barrier, N - 1)
            wo_in.wait()
            gm_in.wait()

        @pl.when(lax.rem(c, PER) == 0)
        def _():
            send_terms(c // PER - 1, group_rows(c // PER - 1), GROUP)

        @pl.when(c == CHUNKS - 2)
        def _():
            send_terms(EARLY, FIRST, HALF)

        @pl.when(jnp.logical_or(c == CHUNKS - 2, jnp.logical_and(lax.rem(c, PER) == PER - 1, jnp.logical_and(c > PER, c < CHUNKS - 1))))
        def _():
            finish_h(c // PER - 1, group_rows(c // PER - 1), GROUP)

        return 0

    lax.fori_loop(1, CHUNKS, chunk, 0)
    v_in(CHUNKS - 1).wait()
    values_of(CHUNKS - 1, p_s[...])
    send_pair()
    finish_h(EARLY, FIRST, HALF)
    lax.fori_loop(0, EARLY - 1, early_h, 0)
    send_chip()
    early_h(EARLY - 1, 0)

    ONE, TWO = pl.ds(0, EARLY * GROUP), pl.ds(EARLY * GROUP, GROUP)

    def hidden(rows, n):
        cols = pl.ds(pl.multiple_of(n * MTILE, MTILE), MTILE)
        gate = dot(a_v[rows, :], wg_v[:, cols])
        up = dot(a_v[rows, :], wu_v[:, cols])
        hid_v[rows, cols] = (jax.nn.silu(gate) * up).astype(BF16)

    wg_in.wait()
    wu_in.wait()
    for n in range(FF // MTILE):
        hidden(ONE, n)
    wd_in.wait()

    in2 = remote(ysend, yrecv, in2_s, in2_r, partner)

    def part_rows(r):
        return pl.ds(r * PART, PART)

    def rs2(r, to):
        return remote(ysum.at[to, part_rows(r)], yfar.at[z, part_rows(r)], rs2_s, rs2_r.at[r], 2 * to + core)

    mine = core * CHIPS + z

    def ag2(r, to):
        b = y_v.at[mine, part_rows(r)]
        return remote(b, b, out2_s, ag2_r.at[r], 2 * to + core)

    def out2(r, source):
        b = y_v.at[core * CHIPS + source, part_rows(r)]
        return remote(b, b, out2_s, out2_r, partner)

    def down(side_of):
        return dot(hid_v[ONE, :], wd_v[:, pl.ds(pl.multiple_of(side_of * CHIPS * COLS, CHIPS * COLS), CHIPS * COLS)])

    def rs3(to):
        return remote(zsend.at[to], zrecv.at[me], rs3_s, rs3_r, to)

    def ag3(to):
        b = y_v.at[me, TWO]
        return remote(b, b, ag3_s, ag3_r, to)

    def finish_part(r):
        rows = part_rows(r)
        total = yown[z, rows, :] + yrecv[z, rows, :].astype(F32)
        arrived(yfar.at[pl.ds(1, CHIPS - 1), rows], rs2_r.at[r])
        for k in range(1, CHIPS):
            total = total + yfar[chip(k), rows, :].astype(F32)
        y_v[mine, rows, :] = (h_v[mine, rows, :].astype(F32) + total).astype(BF16)
        for to in others:
            ag2(r, to).start()
        out2(r, z).start()

    theirs = down(1 - core)
    for q in range(CHIPS):
        ysend[q] = theirs[:, q * COLS:(q + 1) * COLS].astype(BF16)
    in2.start()
    ours = down(core)
    for q in range(CHIPS):
        yown[q] = ours[:, q * COLS:(q + 1) * COLS]
    in2.wait_recv()
    for q in others:
        ysum[q] = (yown[q] + yrecv[q].astype(F32)).astype(BF16)
    for r in range(PARTS):
        for to in others:
            rs2(r, to).start()
    forward_chips()

    arrived(h_v.at[pl.ds(0, N - 1), FIRST], ag_r.at[EARLY])
    last_h()
    norm_h(TWO)
    for n in range(FF // MTILE):
        hidden(TWO, n)
    last = dot(hid_v[TWO, :], wd_v[...])
    for j in range(N):
        block = last[:, j * COLS:(j + 1) * COLS]
        zown[j] = block
        zsend[j] = block.astype(BF16)
    for to in devices:
        rs3(to).start()

    for r in range(PARTS):
        finish_part(r)
    arrived(zrecv.at[pl.ds(1, N - 1)], rs3_r)
    total = zown[me]
    for k in range(1, N):
        total = total + zrecv[peer(k)].astype(F32)
    y_v[me, TWO, :] = (h_v[me, TWO, :].astype(F32) + total).astype(BF16)
    for to in devices:
        ag3(to).start()
    for r in range(PARTS):
        arrived(y_v.at[pl.ds(0, CHIPS - 1), part_rows(r)], ag2_r.at[r])
        for source in others:
            out2(r, source).start()
    arrived(y_v.at[pl.ds(0, CHIPS), ONE], out2_r)
    arrived(y_v.at[pl.ds(0, N - 1), TWO], ag3_r)
    for j in range(N):
        out_h[:, j * COLS:(j + 1) * COLS] = y_v[j]

    for g in range(GROUPS):
        part = pl.ds(0, GROUP if g < EARLY else HALF)
        arrived(tsend.at[g, pl.ds(0, N - 1), part], rs_s.at[g])
        arrived(tsend.at[g, pl.ds(0, N - 1), part], ag_s.at[g])
    pair_copy.wait_send()
    arrived(chips.at[pl.ds(0, CHIPS - 1), half], chip_s)
    arrived(chips.at[pl.ds(0, CHIPS - 1), half], forward_s)
    in2.wait_send()
    arrived(ysum.at[pl.ds(0, CHIPS - 1)], rs2_s)
    arrived(y_v.at[pl.ds(0, N - 1), ONE], out2_s)
    arrived(zsend.at[pl.ds(0, N - 1)], rs3_s)
    arrived(zsend.at[pl.ds(0, N - 1)], ag3_s)


def turns():
    half = HEAD // 2
    angle = (CACHE - 1) * np.float64(THETA) ** (-np.arange(half) / half)
    table = np.stack([np.cos(angle), np.sin(angle)]).astype(np.float32)
    return np.tile(table, (1, 2 * HEADS))


def solution(mesh):
    dma = pltpu.SemaphoreType.DMA

    def step(x, k_cache, v_cache, gain_a, wq, wo, gain_m, w_gate, w_up, w_down):
        k = k_cache.transpose(0, 2, 3, 1).reshape(CHUNKS, SEQS * QD, CACHE)
        v = v_cache.transpose(0, 2, 3, 1).reshape(CHUNKS, SEQS * QD, CACHE)
        vm = pltpu.VMEM
        return pl.pallas_call(
            kernel,
            out_shape=pltpu.VMEM((ROWS, D), BF16),
            in_specs=[pl.BlockSpec(memory_space=pl.ANY)] * 11,
            out_specs=pl.BlockSpec(memory_space=pltpu.VMEM),
            scratch_shapes=[
                vm((ROWS, D), BF16), vm((24, 128), BF16), vm((24, 128), BF16), vm((2, QD), F32),
                vm((D, QD), BF16), vm((QD, D), BF16), vm((D, FF), BF16), vm((D, FF), BF16), vm((FF, D), BF16),
                vm((SLOTS, SEQS * QD, CACHE), BF16), vm((SLOTS, SEQS * QD, CACHE), BF16),
                vm((ROWS, D), BF16), vm((ROWS, QD), F32), vm((SEQS * HEADS, CACHE), BF16), vm((ROWS, QD), F32),
                vm((GROUPS, N, GROUP, COLS), F32), vm((GROUPS, N, GROUP, COLS), BF16), vm((GROUPS, N, GROUP, COLS), BF16),
                vm((N, HALF, COLS), BF16), vm((N, HALF, COLS), BF16), vm((CHIPS, N, HALF, COLS), BF16),
                vm((N, ROWS, COLS), BF16), vm((ROWS, FF), BF16),
                vm((CHIPS, EARLY * GROUP, COLS), BF16), vm((CHIPS, EARLY * GROUP, COLS), BF16), vm((CHIPS, EARLY * GROUP, COLS), F32),
                vm((CHIPS, EARLY * GROUP, COLS), BF16), vm((CHIPS, EARLY * GROUP, COLS), BF16), vm((N, ROWS, COLS), BF16),
                vm((N, GROUP, COLS), F32), vm((N, GROUP, COLS), BF16), vm((N, GROUP, COLS), BF16),
                dma((6,)), dma((SLOTS,)), dma((SLOTS,)), dma((3,)),
                dma((GROUPS,)), dma((GROUPS,)), dma((GROUPS,)), dma((GROUPS,)),
                dma, dma, dma, dma, dma, dma,
                dma, dma, dma, dma((PARTS,)), dma((PARTS,)), dma, dma, dma, dma, dma, dma, dma,
            ],
            compiler_params=pltpu.CompilerParams(collective_id=0, has_side_effects=True, vmem_limit_bytes=58_000_000),
            name="layer",
        )(x, k, v, gain_a.reshape(24, 128), wq, wo, gain_m.reshape(24, 128), w_gate, w_up, w_down, jnp.asarray(turns()))

    states, cache, columns, rows_of = P("dp", None), P("dp", None, "tp", None), P(None, "tp"), P("tp", None)
    return jax.shard_map(
        step,
        mesh=mesh,
        in_specs=(states, cache, cache, P(None), columns, rows_of, P(None), columns, columns, rows_of),
        out_specs=states,
        check_vma=False,
    )
```

```python
import functools

import jax
import jax.numpy as jnp
import numpy as np
from jax import lax
from jax.experimental import pallas as pl
from jax.experimental.pallas import tpu as pltpu
from jax.sharding import PartitionSpec as P

HEAD = 96
THETA = 10000
N = 8
CHIPS = N // 2
ROWS, D = 64, 3072
COLS = D // N
HEADS = 4
QD = HEADS * HEAD
CACHE = 1024
FF = 1024
SEQS = 4
CHUNKS = ROWS // SEQS
SLOTS = 4
GROUP = 16
GROUPS = ROWS // GROUP
EARLY = GROUPS - 1
HALF = GROUP // 2
WIDE = 2
SETS = WIDE + 3
PER = GROUP // SEQS
MTILE = 256
PART = 48
PARTS = EARLY * GROUP // PART
F32, BF16 = jnp.float32, jnp.bfloat16


def dot(a, b):
    return jnp.dot(a, b, preferred_element_type=F32)


def gain_of(ref, start, size):
    rows = range(start // 128, (start + size) // 128)
    return jnp.concatenate([ref[i:i + 1, :].astype(F32) for i in rows], 1)


def kernel(x_h, k_h, v_h, ga_h, wq_h, wo_h, gm_h, wg_h, wu_h, wd_h, cs_h, out_h,
           x_v, ga_v, gm_v, cs_v, wq_v, wo_v, wg_v, wu_v, wd_v, k_v, v_v,
           a_v, q_s, p_s, seen_s, term_s, tsend, trecv, psend, precv, chips, h_v, hid_v,
           ysend, yrecv, yown, ysum, yfar, y_v, zown, zsend, zrecv,
           in_sem, k_sem, v_sem, w_sem, rs_s, rs_r, ag_s, ag_r, pair_s, pair_r, chip_s, chip_r, forward_s, forward_r,
           in2_s, in2_r, rs2_s, rs2_r, ag2_r, out2_s, out2_r, rs3_s, rs3_r, ag3_s, ag3_r):
    me = lax.axis_index("tp")

    z, core = me // 2, lax.rem(me, 2)
    partner = 2 * z + 1 - core

    def peer(k):
        return lax.rem(me + k, N)

    def chip(k):
        return lax.rem(z + k, CHIPS)

    side = z // 2
    edge = z + side * (3 - 2 * z)
    others = [t + side * (3 - 2 * t) for t in (3, 2, 1 - edge)]
    devices = [2 * t + c for t in others for c in (core, 1 - core)] + [partner]

    def arrived(like, sem):
        pltpu.make_async_copy(like, like, sem).wait()

    def remote(src, dst, send_sem, recv_sem, target):
        return pltpu.make_async_remote_copy(
            src_ref=src, dst_ref=dst, send_sem=send_sem, recv_sem=recv_sem,
            device_id={"tp": target}, device_id_type=pl.DeviceIdType.MESH)

    def local(src, dst, sem):
        return pltpu.make_async_copy(src, dst, sem)

    x_in = local(x_h, x_v, in_sem.at[0])
    ga_in = local(ga_h, ga_v, in_sem.at[1])
    cs_in = local(cs_h, cs_v, in_sem.at[2])
    wq_in = local(wq_h, wq_v, in_sem.at[3])
    wo_in = local(wo_h, wo_v, in_sem.at[4])
    gm_in = local(gm_h, gm_v, in_sem.at[5])

    def k_in(c):
        s = lax.rem(c, SLOTS)
        return local(k_h.at[c], k_v.at[s], k_sem.at[s])

    def v_in(c):
        s = lax.rem(c, SLOTS)
        return local(v_h.at[c], v_v.at[s], v_sem.at[s])

    wg_in = local(wg_h, wg_v, w_sem.at[0])
    wu_in = local(wu_h, wu_v, w_sem.at[1])
    wd_in = local(wd_h, wd_v, w_sem.at[2])

    x_in.start()
    ga_in.start()
    cs_in.start()
    wq_in.start()
    for c in range(SLOTS):
        k_in(c).start()
        v_in(c).start()
        if c == 0:
            wo_in.start()
            gm_in.start()

    barrier = pltpu.get_barrier_semaphore()
    for k in range(1, N):
        pl.semaphore_signal(barrier, inc=1, device_id={"tp": peer(k)}, device_id_type=pl.DeviceIdType.MESH)

    x_in.wait()
    ga_in.wait()

    def norm_x(i, _):
        rows = pl.ds(pl.multiple_of(i * GROUP, GROUP), GROUP)
        wide = x_v[rows, :].astype(F32)
        scale = lax.rsqrt(jnp.mean(wide * wide, -1, keepdims=True) + 1e-6)
        a_v[rows, :] = (wide * scale * gain_of(ga_v, 0, D)).astype(BF16)
        return 0

    lax.fori_loop(0, GROUPS, norm_x, 0)
    wq_in.wait()
    cs_in.wait()
    q = dot(a_v[...], wq_v[...]).astype(BF16).astype(F32)
    lane = lax.broadcasted_iota(jnp.int32, (ROWS, QD), 1)
    ahead = pltpu.roll(q, QD - HEAD // 2, 1)
    behind = pltpu.roll(q, HEAD // 2, 1)
    turn = jnp.where(lax.rem(lane, HEAD) < HEAD // 2, -ahead, behind)
    q_s[...] = (q * cs_v[0:1, :] + turn * cs_v[1:2, :]).astype(BF16).astype(F32)

    row16 = lax.broadcasted_iota(jnp.int32, (SEQS * HEADS, QD), 0)
    lane16 = lax.broadcasted_iota(jnp.int32, (SEQS * HEADS, QD), 1)
    masks = [row16 == i * HEADS + lane16 // HEAD for i in range(SEQS)]

    def weights_of(c):
        k_in(c).wait()
        parts = []
        for i in range(SEQS):
            row = q_s[pl.ds(c * SEQS + i, 1), :]
            parts.append(jnp.where(masks[i], jnp.broadcast_to(row, (SEQS * HEADS, QD)), 0.0))
        qd = jnp.concatenate(parts, 1).astype(BF16)
        s = dot(qd, k_v[lax.rem(c, SLOTS)]) * HEAD**-0.5
        e = jnp.exp(s - jnp.max(s, -1, keepdims=True))
        return (e * (1.0 / jnp.sum(e, -1, keepdims=True))).astype(BF16)

    def values_of(c, p):
        o = lax.dot_general(p, v_v[lax.rem(c, SLOTS)], (((1,), (1,)), ((), ())), preferred_element_type=F32)
        for i in range(SEQS):
            part = jnp.where(masks[i], o[:, i * QD:(i + 1) * QD], 0.0)
            seen_s[pl.ds(c * SEQS + i, 1), :] = jnp.sum(part, 0, keepdims=True)

    def group_rows(g):
        return pl.ds(pl.multiple_of(g * GROUP, GROUP), GROUP)

    def rs_copy(g, to, size):
        part = pl.ds(0, size)
        return remote(tsend.at[g, to, part], trecv.at[g, me, part], rs_s.at[g], rs_r.at[g], to)

    def ag_copy(g, to, rows):
        block = h_v.at[me, rows, :]
        return remote(block, block, ag_s.at[g], ag_r.at[g], to)

    FIRST, LAST = (pl.ds(EARLY * GROUP + t * HALF, HALF) for t in range(2))

    def narrow(g):
        return pl.ds(WIDE * GROUP + (g - WIDE) * HALF, HALF)

    def send_terms(g, rows, size):
        term = dot(seen_s[rows, :].astype(BF16), wo_v[...])
        for j in range(N):
            block = term[:, j * COLS:(j + 1) * COLS]
            term_s[g, j, :size] = block
            tsend[g, j, :size] = block.astype(BF16)
        for to in devices:
            rs_copy(g, to, size).start()

    def finish_h(g, rows, size):
        arrived(trecv.at[g, pl.ds(1, N - 1), pl.ds(0, size)], rs_r.at[g])
        total = term_s[g, me, :size]
        for k in range(1, N):
            total = total + trecv[g, peer(k), :size].astype(F32)
        mine = x_v[rows, pl.ds(pl.multiple_of(me * COLS, COLS), COLS)].astype(F32)
        h_v[me, rows, :] = (mine + total).astype(BF16)
        for to in devices:
            ag_copy(g, to, rows).start()

    def norm_h(rows):
        wide = [h_v[j, rows, :].astype(F32) for j in range(N)]
        square = sum(jnp.sum(w * w, -1, keepdims=True) for w in wide)
        scale = lax.rsqrt(square / D + 1e-6)
        for j in range(N):
            cols = slice(j * COLS, (j + 1) * COLS)
            a_v[rows, cols] = (wide[j] * scale * gain_of(gm_v, j * COLS, COLS)).astype(BF16)

    def early_h(g, _):
        arrived(h_v.at[pl.ds(0, N - 1), group_rows(g)], ag_r.at[g])
        norm_h(group_rows(g))
        return 0

    pair_copy = remote(psend, precv, pair_s, pair_r, partner)

    half = pl.ds(core * CHIPS, CHIPS)

    def chip_copy(to):
        return remote(chips.at[z, half], chips.at[z, half], chip_s, chip_r, 2 * to + core)

    def forward_copy(source):
        return remote(chips.at[source, half], chips.at[source, half], forward_s, forward_r, partner)

    def send_pair():
        term = dot(seen_s[LAST, :].astype(BF16), wo_v[...])
        for j in range(N):
            psend[j] = term[:, j * COLS:(j + 1) * COLS].astype(BF16)
        pair_copy.start()

    def send_chip():
        pair_copy.wait_recv()
        chips[z] = (psend[...].astype(F32) + precv[...].astype(F32)).astype(BF16)
        for to in others:
            chip_copy(to).start()

    def forward_chips():
        arrived(chips.at[pl.ds(0, CHIPS - 1), half], chip_r)
        for source in others:
            forward_copy(source).start()

    def last_h():
        arrived(chips.at[pl.ds(0, CHIPS - 1), half], forward_r)
        for j in range(N):
            total = x_v[LAST, j * COLS:(j + 1) * COLS].astype(F32)
            for q in range(CHIPS):
                total = total + chips[q, j].astype(F32)
            h_v[j, LAST, :] = total.astype(BF16)

    p_s[...] = weights_of(0)
    def chunk(c, _):
        @pl.when(c + SLOTS - 1 < CHUNKS)
        def _():
            k_in(c + SLOTS - 1).start()

        @pl.when(jnp.logical_and(c >= 2, c + SLOTS - 2 < CHUNKS))
        def _():
            v_in(c + SLOTS - 2).start()

        @pl.when(c == CHUNKS - SLOTS + 1)
        def _():
            for w in (wg_in, wu_in, wd_in):
                w.start(priority=1)

        v_in(c - 1).wait()
        p = p_s[...]
        p_s[...] = weights_of(c)
        values_of(c - 1, p)

        @pl.when(c == PER)
        def _():
            pl.semaphore_wait(barrier, N - 1)
            wo_in.wait()
            gm_in.wait()

        @pl.when(jnp.logical_and(lax.rem(c, PER) == 0, c <= WIDE * PER))
        def _():
            send_terms(c // PER - 1, group_rows(c // PER - 1), GROUP)

        for g in range(WIDE, SETS):
            @pl.when(c == (g - WIDE) * PER // 2 + WIDE * PER + PER // 2)
            def _(g=g):
                send_terms(g, narrow(g), HALF)

        @pl.when(jnp.logical_and(lax.rem(c, PER) == PER - 1, jnp.logical_and(c > PER, c <= WIDE * PER + PER - 1)))
        def _():
            finish_h(c // PER - 1, group_rows(c // PER - 1), GROUP)

        for g, at in ((WIDE, CHUNKS - 3), (WIDE + 1, CHUNKS - 2)):
            @pl.when(c == at)
            def _(g=g):
                finish_h(g, narrow(g), HALF)

        return 0

    lax.fori_loop(1, CHUNKS, chunk, 0)
    v_in(CHUNKS - 1).wait()
    values_of(CHUNKS - 1, p_s[...])
    send_pair()
    finish_h(SETS - 1, FIRST, HALF)
    lax.fori_loop(0, WIDE, early_h, 0)
    send_chip()
    for g in (WIDE, WIDE + 1):
        arrived(h_v.at[pl.ds(0, N - 1), narrow(g)], ag_r.at[g])
    norm_h(group_rows(WIDE))

    ONE, TWO = pl.ds(0, EARLY * GROUP), pl.ds(EARLY * GROUP, GROUP)

    def hidden(rows, n):
        cols = pl.ds(pl.multiple_of(n * MTILE, MTILE), MTILE)
        gate = dot(a_v[rows, :], wg_v[:, cols])
        up = dot(a_v[rows, :], wu_v[:, cols])
        hid_v[rows, cols] = (jax.nn.silu(gate) * up).astype(BF16)

    wg_in.wait()
    wu_in.wait()
    for n in range(FF // MTILE):
        hidden(ONE, n)
    wd_in.wait()

    in2 = remote(ysend, yrecv, in2_s, in2_r, partner)

    def part_rows(r):
        return pl.ds(r * PART, PART)

    def rs2(r, to):
        return remote(ysum.at[to, part_rows(r)], yfar.at[z, part_rows(r)], rs2_s, rs2_r.at[r], 2 * to + core)

    mine = core * CHIPS + z

    def ag2(r, to):
        b = y_v.at[mine, part_rows(r)]
        return remote(b, b, out2_s, ag2_r.at[r], 2 * to + core)

    def out2(r, source):
        b = y_v.at[core * CHIPS + source, part_rows(r)]
        return remote(b, b, out2_s, out2_r, partner)

    def down(side_of):
        return dot(hid_v[ONE, :], wd_v[:, pl.ds(pl.multiple_of(side_of * CHIPS * COLS, CHIPS * COLS), CHIPS * COLS)])

    def rs3(to):
        return remote(zsend.at[to], zrecv.at[me], rs3_s, rs3_r, to)

    def ag3(to):
        b = y_v.at[me, TWO]
        return remote(b, b, ag3_s, ag3_r, to)

    def finish_part(r):
        rows = part_rows(r)
        total = yown[z, rows, :] + yrecv[z, rows, :].astype(F32)
        arrived(yfar.at[pl.ds(1, CHIPS - 1), rows], rs2_r.at[r])
        for k in range(1, CHIPS):
            total = total + yfar[chip(k), rows, :].astype(F32)
        y_v[mine, rows, :] = (h_v[mine, rows, :].astype(F32) + total).astype(BF16)
        for to in others:
            ag2(r, to).start()
        out2(r, z).start()

    theirs = down(1 - core)
    for q in range(CHIPS):
        ysend[q] = theirs[:, q * COLS:(q + 1) * COLS].astype(BF16)
    in2.start()
    ours = down(core)
    for q in range(CHIPS):
        yown[q] = ours[:, q * COLS:(q + 1) * COLS]
    in2.wait_recv()
    for q in others:
        ysum[q] = (yown[q] + yrecv[q].astype(F32)).astype(BF16)
    for r in range(PARTS):
        for to in others:
            rs2(r, to).start()
    forward_chips()

    arrived(h_v.at[pl.ds(0, N - 1), FIRST], ag_r.at[SETS - 1])
    last_h()
    norm_h(TWO)
    for n in range(FF // MTILE):
        hidden(TWO, n)
    last = dot(hid_v[TWO, :], wd_v[...])
    for j in range(N):
        block = last[:, j * COLS:(j + 1) * COLS]
        zown[j] = block
        zsend[j] = block.astype(BF16)
    for to in devices:
        rs3(to).start()

    for r in range(PARTS):
        finish_part(r)
    arrived(zrecv.at[pl.ds(1, N - 1)], rs3_r)
    total = zown[me]
    for k in range(1, N):
        total = total + zrecv[peer(k)].astype(F32)
    y_v[me, TWO, :] = (h_v[me, TWO, :].astype(F32) + total).astype(BF16)
    for to in devices:
        ag3(to).start()
    for r in range(PARTS):
        arrived(y_v.at[pl.ds(0, CHIPS - 1), part_rows(r)], ag2_r.at[r])
        for source in others:
            out2(r, source).start()
    arrived(y_v.at[pl.ds(0, CHIPS), ONE], out2_r)
    arrived(y_v.at[pl.ds(0, N - 1), TWO], ag3_r)
    for j in range(N):
        out_h[:, j * COLS:(j + 1) * COLS] = y_v[j]

    for g in range(SETS):
        part = pl.ds(0, GROUP if g < WIDE else HALF)
        arrived(tsend.at[g, pl.ds(0, N - 1), part], rs_s.at[g])
        arrived(tsend.at[g, pl.ds(0, N - 1), part], ag_s.at[g])
    pair_copy.wait_send()
    arrived(chips.at[pl.ds(0, CHIPS - 1), half], chip_s)
    arrived(chips.at[pl.ds(0, CHIPS - 1), half], forward_s)
    in2.wait_send()
    arrived(ysum.at[pl.ds(0, CHIPS - 1)], rs2_s)
    arrived(y_v.at[pl.ds(0, N - 1), ONE], out2_s)
    arrived(zsend.at[pl.ds(0, N - 1)], rs3_s)
    arrived(zsend.at[pl.ds(0, N - 1)], ag3_s)


def turns():
    half = HEAD // 2
    angle = (CACHE - 1) * np.float64(THETA) ** (-np.arange(half) / half)
    table = np.stack([np.cos(angle), np.sin(angle)]).astype(np.float32)
    return np.tile(table, (1, 2 * HEADS))


def solution(mesh):
    dma = pltpu.SemaphoreType.DMA

    def step(x, k_cache, v_cache, gain_a, wq, wo, gain_m, w_gate, w_up, w_down):
        k = k_cache.transpose(0, 2, 3, 1).reshape(CHUNKS, SEQS * QD, CACHE)
        v = v_cache.transpose(0, 2, 3, 1).reshape(CHUNKS, SEQS * QD, CACHE)
        vm = pltpu.VMEM
        return pl.pallas_call(
            kernel,
            out_shape=pltpu.VMEM((ROWS, D), BF16),
            in_specs=[pl.BlockSpec(memory_space=pl.ANY)] * 11,
            out_specs=pl.BlockSpec(memory_space=pltpu.VMEM),
            scratch_shapes=[
                vm((ROWS, D), BF16), vm((24, 128), BF16), vm((24, 128), BF16), vm((2, QD), F32),
                vm((D, QD), BF16), vm((QD, D), BF16), vm((D, FF), BF16), vm((D, FF), BF16), vm((FF, D), BF16),
                vm((SLOTS, SEQS * QD, CACHE), BF16), vm((SLOTS, SEQS * QD, CACHE), BF16),
                vm((ROWS, D), BF16), vm((ROWS, QD), F32), vm((SEQS * HEADS, CACHE), BF16), vm((ROWS, QD), F32),
                vm((SETS, N, GROUP, COLS), F32), vm((SETS, N, GROUP, COLS), BF16), vm((SETS, N, GROUP, COLS), BF16),
                vm((N, HALF, COLS), BF16), vm((N, HALF, COLS), BF16), vm((CHIPS, N, HALF, COLS), BF16),
                vm((N, ROWS, COLS), BF16), vm((ROWS, FF), BF16),
                vm((CHIPS, EARLY * GROUP, COLS), BF16), vm((CHIPS, EARLY * GROUP, COLS), BF16), vm((CHIPS, EARLY * GROUP, COLS), F32),
                vm((CHIPS, EARLY * GROUP, COLS), BF16), vm((CHIPS, EARLY * GROUP, COLS), BF16), vm((N, ROWS, COLS), BF16),
                vm((N, GROUP, COLS), F32), vm((N, GROUP, COLS), BF16), vm((N, GROUP, COLS), BF16),
                dma((6,)), dma((SLOTS,)), dma((SLOTS,)), dma((3,)),
                dma((SETS,)), dma((SETS,)), dma((SETS,)), dma((SETS,)),
                dma, dma, dma, dma, dma, dma,
                dma, dma, dma, dma((PARTS,)), dma((PARTS,)), dma, dma, dma, dma, dma, dma,
            ],
            compiler_params=pltpu.CompilerParams(collective_id=0, has_side_effects=True, vmem_limit_bytes=58_000_000),
            name="layer",
        )(x, k, v, gain_a.reshape(24, 128), wq, wo, gain_m.reshape(24, 128), w_gate, w_up, w_down, jnp.asarray(turns()))

    states, cache, columns, rows_of = P("dp", None), P("dp", None, "tp", None), P(None, "tp"), P("tp", None)
    return jax.shard_map(
        step,
        mesh=mesh,
        in_specs=(states, cache, cache, P(None), columns, rows_of, P(None), columns, columns, rows_of),
        out_specs=states,
        check_vma=False,
    )
```
